256 devices in a mesh: row: 16 (over x, y), col: 8 (over z), depth: 2 (over core).
Axes of the slice: x: 4, y: 4, z: 8, core: 2. Of those that a mesh axis runs over, the one named last changes fastest.
Arguments:
- halves: bfloat16 [2, 8192, 16384], P(None, 'row', ('col', 'depth')), may hold values from -6 to 6
- spectrum: float32 [2, 16384], P(None, ('col', 'depth')), as said below
- wanted: int32 [4096], P('col'), may hold values from 0 to 32766, as said below
- fraction: float32 [4096], P('col'), may hold values from 0.05 to 0.95
Outputs:
- eigvec: float32 [2, 8192, 4096], P(None, 'row', ('col', 'depth'))
The draws below stay inside these ranges and needn't reach their ends.
Inputs may be any that keep to these rules, and one draw needn't show every extreme that they name: Read in the order spectrum[0,0], spectrum[1,0], spectrum[0,1], spectrum[1,1], ... the values rise strictly, each by more than 0.05 over the one before. `wanted`: distinct positions in that merged order of the 32768 eigenvalues.
All inputs are finite; a program needn't handle non-finite values.
Results may differ from the reference program's by a relative error of at most 0.0029.
Values may be sent and summed in bfloat16 or wider, within the bound.
A program may use at most 128 MiB of HBM per device.

```python
import math
import jax
import jax.numpy as jnp
from jax import lax

H = 16384
R = 8192
K = 4096


def draw_halves(key, part):
    noise_key = jax.random.fold_in(key, 11)
    random_part = jnp.clip(jax.random.normal(noise_key, (2, R, H), jnp.float32), -6.0, 6.0)
    values = random_part
    return values.astype(jnp.bfloat16)


def draw_spectrum(key, part):
    gaps = jnp.exp(jax.random.uniform(key, (2 * H,), jnp.float32, math.log(0.5), math.log(2.0)))
    ordered = jnp.cumsum(gaps)
    ordered = ordered - 0.5 * ordered[-1]
    return ordered.reshape(H, 2).T.astype(jnp.float32)


def draw_wanted(key, part):
    return jax.random.permutation(key, 2 * H - 1)[:K].astype(jnp.int32)


def level_of(key, extent, pieces, low, top_value):
    gain = 1.0
    for position, blocks in pieces:
        draws = jax.random.uniform(jax.random.fold_in(jax.random.fold_in(key, 6), position), (blocks,), jnp.float32, low / len(pieces), top_value / len(pieces))
        gain = gain * jnp.repeat(jnp.exp(draws), extent[position] // blocks).reshape((-1,) + (1,) * (len(extent) - 1 - position))
    return gain


def setup_inputs(seed: int = 0) -> dict:
    arg_keys = jax.random.split(jax.random.key(seed), 5)
    return {
        "halves": draw_halves(jax.random.fold_in(arg_keys[4], 71), 0),
        "spectrum": draw_spectrum(jax.random.fold_in(arg_keys[4], 71), 0),
        "wanted": draw_wanted(jax.random.fold_in(arg_keys[4], 71), 0),
        "fraction": jnp.clip(0.05 + 0.9 * jax.random.uniform(arg_keys[3], (K,), jnp.float32) ** level_of(arg_keys[3], (K,), ((0, 8),), -0.2, 0.2), 0.05, 0.95),
    }


def root_terms(spectrum, wanted):
    ordered = jnp.stack([spectrum[0], spectrum[1]], axis=1).reshape(-1)
    lower = jnp.take(ordered, wanted)
    upper = jnp.take(ordered, wanted + 1)
    return (lower, upper - lower)

def reference(halves, spectrum, wanted, fraction):
    seam = jnp.stack([halves[0, R - 1], halves[1, 0]]).astype(jnp.float32)
    lower, width = root_terms(spectrum, wanted)
    block = math.gcd(K, 512)
    count = K // block

    def one(index):
        start = (index * block).astype(jnp.int32)
        low = lax.dynamic_slice_in_dim(lower, start, block)
        wid = lax.dynamic_slice_in_dim(width, start, block)
        frc = lax.dynamic_slice_in_dim(fraction, start, block)
        cauchy = seam[:, :, None] / (spectrum[:, :, None] - low[None, None, :] - frc[None, None, :] * wid[None, None, :])
        norms = jnp.sqrt(lax.optimization_barrier(jnp.sum(cauchy * cauchy, axis=(0, 1))))
        rounded = cauchy.astype(jnp.bfloat16)
        first = jnp.dot(halves[0], rounded[0], preferred_element_type=jnp.float32)
        second = jnp.dot(halves[1], rounded[1], preferred_element_type=jnp.float32)
        return jnp.stack([first, second]) / norms[None, None, :]
    result = lax.map(one, jnp.arange(count).astype(jnp.int32))
    return jnp.transpose(result, (1, 2, 0, 3)).reshape(2, R, K)
```

```python
import functools

import jax
import jax.numpy as jnp
from jax import lax
from jax.experimental import pallas as pl
from jax.experimental.pallas import tpu as pltpu
from jax.sharding import PartitionSpec as P

MESH = pl.DeviceIdType.MESH
LANES = 128


def log2(x):
    return x.bit_length() - 1


def kernel(
    nrow,
    n,
    halves,
    pay,
    out,
    afull,
    tab,
    seam,
    tcat,
    ct,
    part,
    sbuf,
    rbuf,
    ssq,
    ssq_s,
    ssq_r,
    lowb,
    fwb,
    a_sem,
    tab_send,
    tab_recv,
    seam_send,
    seam_recv,
    ring_send,
    ring_recv,
    ssq_send,
    ssq_recv,
):
    row, z, c = lax.axis_index("row"), lax.axis_index("col"), lax.axis_index("depth")
    rows, width = halves.shape[1], halves.shape[2]
    tiles = width // LANES
    cols = out.shape[2]
    kblocks = cols // LANES
    half = rows // 2
    me = z * 2 + c
    other = 1 - c
    first, last = row == 0, row == nrow - 1
    edge = jnp.logical_or(first, last)

    def copy_out(src, dst, send, recv, where):
        return pltpu.make_async_remote_copy(
            src_ref=src, dst_ref=dst, send_sem=send, recv_sem=recv, device_id=where, device_id_type=MESH
        )

    a_local = pltpu.make_async_copy(halves, afull.at[c], a_sem.at[0])
    a_local.start()
    tab_local = pltpu.make_async_copy(pay.at[pl.ds(2, 3)], tab.at[me], tab_recv.at[me])
    tab_local.start()

    barrier = pltpu.get_barrier_semaphore()

    def greet(where):
        pl.semaphore_signal(barrier, inc=1, device_id=where, device_id_type=MESH)

    for o in range(1, n):
        zz = lax.rem(z + o, n)
        greet((row, zz, c))
        greet((row, zz, other))
    greet((row, z, other))

    @pl.when(edge)
    def _():
        def one(i, carry):
            rr = lax.rem(row + i, nrow)
            greet((rr, z, c))
            greet((rr, z, other))
            return carry

        lax.fori_loop(1, nrow, one, 0)

    @pl.when(jnp.logical_not(edge))
    def _():
        for rr in (0, nrow - 1):
            greet((rr, z, c))
            greet((rr, z, other))

    pl.semaphore_wait(barrier, 2 * n - 1 + jnp.where(edge, 2 * (nrow - 1), 4))

    def tab_same(o):
        return copy_out(
            pay.at[pl.ds(2, 3)], tab.at[me], tab_send.at[o], tab_recv.at[me], (row, lax.rem(z + o, n), c)
        )

    def tab_other(o):
        return copy_out(
            pay.at[pl.ds(2, 2)],
            tab.at[me, pl.ds(0, 2)],
            tab_send.at[n + o],
            tab_recv.at[me],
            (row, lax.rem(z + o, n), other),
        )

    order = sorted(range(1, n), key=lambda o: -min(o, n - o))
    for o in order:
        tab_same(o).start()
        tab_other(o).start()
    tab_other(0).start()

    def seam_copy(a, i, where_c):
        return copy_out(
            pay.at[a],
            seam.at[c, a],
            seam_send.at[2 * i + where_c],
            seam_recv.at[c, a],
            (lax.rem(row + i, nrow), z, where_c),
        )

    def seam_sends(a, act):
        def one(i, carry):
            act(seam_copy(a, i, 0))
            act(seam_copy(a, i, 1))
            return carry

        lax.fori_loop(1, nrow, one, 0)
        act(copy_out(pay.at[a], seam.at[c, a], seam_send.at[0], seam_recv.at[c, a], (row, z, other)))

    for flag, a in ((last, 0), (first, 1)):

        @pl.when(flag)
        def _(a=a):
            pltpu.make_async_copy(pay.at[a], seam.at[c, a], seam_recv.at[c, a]).start()
            seam_sends(a, lambda d: d.start())

    a_swap = copy_out(halves, afull.at[c], a_sem.at[1], a_sem.at[2], (row, z, other))
    a_swap.start()

    for o in range(n):
        zz = lax.rem(z + o, n)
        g = zz * 2 + c
        pltpu.make_async_copy(tab.at[g], tab.at[g], tab_recv.at[g]).wait()
        g = zz * 2 + other
        pltpu.make_async_copy(tab.at[g, pl.ds(0, 2)], tab.at[g, pl.ds(0, 2)], tab_recv.at[g]).wait()

    table = tab[:, 0:2].reshape(2 * n * 2 * tiles, LANES) * 0.25
    hi = table.astype(jnp.bfloat16)
    rest = table - hi.astype(jnp.float32)
    mid = rest.astype(jnp.bfloat16)
    low = (rest - mid.astype(jnp.float32)).astype(jnp.bfloat16)
    tcat[:, 0:LANES] = hi
    tcat[:, LANES : 2 * LANES] = mid
    tcat[:, 2 * LANES : 3 * LANES] = low

    def pick(position):
        h = lax.shift_right_logical(position, 1)
        a = position & 1
        g = lax.shift_right_logical(h, log2(width))
        s = lax.shift_right_logical(h, log2(LANES)) & (tiles - 1)
        entry = (g * 2 + a) * tiles + s
        lane = h & (LANES - 1)
        table_rows = tcat.shape[0]
        hit = lax.broadcasted_iota(jnp.int32, (cols, table_rows), 1) == entry
        onehot = jnp.where(hit, 1.0, 0.0).astype(jnp.bfloat16)
        found = jnp.dot(onehot, tcat[...], preferred_element_type=jnp.float32)
        value = (found[:, 0:LANES] + found[:, LANES : 2 * LANES]) + found[:, 2 * LANES : 3 * LANES]
        here = lax.broadcasted_iota(jnp.int32, (cols, LANES), 1) == lane
        return jnp.sum(jnp.where(here, value, 0.0), axis=1, keepdims=True) * 4.0

    def roots(d):
        wf = tab[d * 2 + c, 2].T
        need = 2 * kblocks

        def column(at):
            got = [
                jnp.where(c == 0, wf[:, at + b : at + b + 1], wf[:, at + kblocks + b : at + kblocks + b + 1])
                for b in range(kblocks)
            ]
            return jnp.concatenate(got, axis=0)

        position = column(0).astype(jnp.int32)
        frac = column(need)
        lower = pick(position)
        upper = pick(position + 1)
        lowb[...] = jnp.broadcast_to(lower, lowb.shape)
        fwb[...] = jnp.broadcast_to(frac * (upper - lower), fwb.shape)

    def at_offset(off):
        return lax.rem(z + off + n, n)

    def ssq_copy(off):
        d = at_offset(off)
        return copy_out(
            ssq_s.at[off % n], ssq_r.at[z], ssq_send.at[off % n], ssq_recv.at[z], (row, d, c)
        )

    def cauchy(a):
        def one(t, carry):
            dp, s = t // tiles, lax.rem(t, tiles)
            value = tab[z * 2 + dp, a, pl.ds(s, 1), :]
            weight = seam[dp, a, pl.ds(s, 1), :]
            term = weight / ((value - lowb[...]) - fwb[...])
            ssq[...] += term * term
            ct[:, pl.ds(pl.multiple_of(t * LANES, LANES), LANES)] = term.astype(jnp.bfloat16)
            return carry

        lax.fori_loop(0, 2 * tiles, one, 0)

    def product(slot, a):
        dims = (((1,), (1,)), ((), ()))
        part[slot, a] = lax.dot_general(
            afull[0, a], ct[:, 0:width], dims, preferred_element_type=jnp.float32
        ) + lax.dot_general(afull[1, a], ct[:, width : 2 * width], dims, preferred_element_type=jnp.float32)

    def compute(off):
        roots(at_offset(off))
        ssq[...] = jnp.zeros_like(ssq)

        def one(a, carry):
            cauchy(a)
            product(off % n, a)
            return carry

        lax.fori_loop(0, 2, one, 0)
        line = jnp.sum(ssq[...].T, axis=0, keepdims=True)
        for b in range(kblocks):
            ssq_s[off % n, b : b + 1, :] = line[:, b * LANES : (b + 1) * LANES]

    steps = n - 1

    def ring_copy(j, way, a):
        step = 1 if way == 0 else n - 1
        return copy_out(
            sbuf.at[j, way, a],
            rbuf.at[j, way, a],
            ring_send.at[j, way, a],
            ring_recv.at[j, way, a],
            (row, lax.rem(z + step, n), c),
        )

    def offset_of(j, way):
        off = n // 2 - (j + 1) // 2
        return off if way == 0 else -off

    def half_of(j, way):
        return (j + way) % 2

    def mine(j, way, a):
        off, hh = offset_of(j, way), half_of(j, way)
        return part[off % n, a, hh * half : (hh + 1) * half, :]

    def launch(j, way):
        for a in range(2):
            sbuf[j, way, a] = mine(j, way, a).astype(jnp.bfloat16)
            ring_copy(j, way, a).start()

    def relay(j):
        for a in range(2):
            for way in range(2):
                ring_copy(j - 2, way, a).wait_recv()
                total = mine(j, way, a) + rbuf[j - 2, way, a].astype(jnp.float32)
                sbuf[j, way, a] = total.astype(jnp.bfloat16)
                ring_copy(j, way, a).start()

    for cc in range(2):
        for a in range(2):
            pltpu.make_async_copy(seam.at[cc, a], seam.at[cc, a], seam_recv.at[cc, a]).wait()
    a_local.wait()
    a_swap.wait_recv()

    m = n // 2
    plan = [m]
    for off in range(m - 1, 0, -1):
        plan += [off, -off]
    plan.append(0)
    done_relay = 2
    for i, off in enumerate(plan):
        compute(off)
        if off != 0:
            ssq_copy(off).start()
        if i == 0:
            launch(0, 0)
            launch(0, 1)
        elif i == 1:
            launch(1, 0)
        elif i == 2:
            launch(1, 1)
        elif i >= 4 and i % 2 == 0 and done_relay < steps:
            relay(done_relay)
            done_relay += 1
    for j in range(done_relay, steps):
        relay(j)

    total = ssq_s[0]
    for o in range(1, n):
        zz = lax.rem(z + o, n)
        pltpu.make_async_copy(ssq_r.at[zz], ssq_r.at[zz], ssq_recv.at[zz]).wait()
        total = total + ssq_r[zz]
    norm = jnp.sqrt(total)
    norm = jnp.concatenate([norm[b : b + 1] for b in range(kblocks)], axis=1)
    for hh in range(2):
        for a in range(2):
            value = part[0, a, hh * half : (hh + 1) * half, :]
            for way in range(2):
                j = steps - 2 + (hh + way + steps) % 2
                ring_copy(j, way, a).wait_recv()
                value = value + rbuf[j, way, a].astype(jnp.float32)
            out[a, hh * half : (hh + 1) * half, :] = value / norm

    for o in order:
        tab_same(o).wait_send()
        tab_other(o).wait_send()
    tab_other(0).wait_send()
    for flag, a in ((last, 0), (first, 1)):

        @pl.when(flag)
        def _(a=a):
            seam_sends(a, lambda d: d.wait_send())

    a_swap.wait_send()
    for off in plan[:-1]:
        ssq_copy(off).wait_send()
    for j in range(steps):
        for way in range(2):
            for a in range(2):
                ring_copy(j, way, a).wait_send()


def merge(nrow, n, halves, spectrum, wanted, fraction):
    rows, width = halves.shape[1:]
    tiles = width // LANES
    cols = wanted.shape[0] // 2
    seam = jnp.stack([halves[0, rows - 1], halves[1, 0]]).astype(jnp.float32)
    pay = jnp.concatenate(
        [
            seam.reshape(2, tiles, LANES),
            spectrum.reshape(2, tiles, LANES),
            jnp.concatenate([wanted.astype(jnp.float32), fraction]).reshape(1, 4 * cols // LANES, LANES),
        ],
        axis=0,
    )
    half = rows // 2
    steps = n - 1
    bf16, f32 = jnp.bfloat16, jnp.float32
    return pl.pallas_call(
        functools.partial(kernel, nrow, n),
        out_shape=jax.ShapeDtypeStruct((2, rows, cols), f32),
        in_specs=[pl.BlockSpec(memory_space=pl.ANY), pl.BlockSpec(memory_space=pltpu.VMEM)],
        out_specs=pl.BlockSpec(memory_space=pltpu.VMEM),
        scratch_shapes=[
            pltpu.VMEM((2, 2, rows, width), bf16),
            pltpu.VMEM((2 * n, 3, tiles, LANES), f32),
            pltpu.VMEM((2, 2, tiles, LANES), f32),
            pltpu.VMEM((2 * n * 2 * tiles, 3 * LANES), bf16),
            pltpu.VMEM((cols, 2 * width), bf16),
            pltpu.VMEM((n, 2, rows, cols), f32),
            pltpu.VMEM((steps, 2, 2, half, cols), bf16),
            pltpu.VMEM((steps, 2, 2, half, cols), bf16),
            pltpu.VMEM((cols, LANES), f32),
            pltpu.VMEM((n, cols // LANES, LANES), f32),
            pltpu.VMEM((n, cols // LANES, LANES), f32),
            pltpu.VMEM((cols, LANES), f32),
            pltpu.VMEM((cols, LANES), f32),
            pltpu.SemaphoreType.DMA((3,)),
            pltpu.SemaphoreType.DMA((2 * n,)),
            pltpu.SemaphoreType.DMA((2 * n,)),
            pltpu.SemaphoreType.DMA((2 * nrow,)),
            pltpu.SemaphoreType.DMA((2, 2)),
            pltpu.SemaphoreType.DMA((steps, 2, 2)),
            pltpu.SemaphoreType.DMA((steps, 2, 2)),
            pltpu.SemaphoreType.DMA((n,)),
            pltpu.SemaphoreType.DMA((n,)),
        ],
        compiler_params=pltpu.CompilerParams(
            collective_id=0, has_side_effects=True, vmem_limit_bytes=48 * 1024 * 1024
        ),
        name="merge",
    )(halves, pay)


def solution(mesh):
    body = functools.partial(merge, mesh.shape["row"], mesh.shape["col"])
    in_specs = (P(None, "row", ("col", "depth")), P(None, ("col", "depth")), P("col"), P("col"))
    out_specs = P(None, "row", ("col", "depth"))
    return jax.shard_map(body, mesh=mesh, in_specs=in_specs, out_specs=out_specs, check_vma=False)
```

```python
import functools

import jax
import jax.numpy as jnp
from jax import lax
from jax.experimental import pallas as pl
from jax.experimental.pallas import tpu as pltpu
from jax.sharding import PartitionSpec as P

MESH = pl.DeviceIdType.MESH
LANES = 128


def log2(x):
    return x.bit_length() - 1


def kernel(
    nrow,
    n,
    halves,
    spectrum,
    wanted,
    fraction,
    out,
    afull,
    edges,
    edge_row,
    tab,
    near,
    want,
    frac,
    seam,
    specb,
    seamb,
    tcat,
    ct,
    part,
    sbuf,
    rbuf,
    ssq_s,
    ssq_r,
    a_sem,
    local_sem,
    tab_sem,
    want_sem,
    frac_sem,
    seam_send,
    seam_recv,
    ring_send,
    ring_recv,
    ssq_sem,
):
    row, z, c = lax.axis_index("row"), lax.axis_index("col"), lax.axis_index("depth")
    rows, width = halves.shape[1], halves.shape[2]
    tiles = width // LANES
    cols = out.shape[2]
    kblocks = cols // LANES
    half = rows // 2
    other = 1 - c
    first, last = row == 0, row == nrow - 1
    edge = jnp.logical_or(first, last)

    def copy_out(src, dst, send, recv, where):
        return pltpu.make_async_remote_copy(
            src_ref=src, dst_ref=dst, send_sem=send, recv_sem=recv, device_id=where, device_id_type=MESH
        )

    own = pl.ds(pl.multiple_of(c * width, width), width)
    sources = [
        (spectrum.at[:, 0], tab.at[c, z, 0]),
        (spectrum.at[:, 1], tab.at[c, z, 1]),
        (wanted.at[c], want.at[z]),
        (fraction.at[c], frac.at[z]),
        (halves.at[0, pl.ds(rows - 8, 8)], edges.at[0]),
        (halves.at[1, pl.ds(0, 8)], edges.at[1]),
    ]
    local = [pltpu.make_async_copy(src, dst, local_sem.at[k]) for k, (src, dst) in enumerate(sources)]
    for d in local:
        d.start()
    a_local = pltpu.make_async_copy(halves, afull.at[:, :, own], a_sem.at[0])
    a_local.start()

    barrier = pltpu.get_barrier_semaphore()

    def greet(where):
        pl.semaphore_signal(barrier, inc=1, device_id=where, device_id_type=MESH)

    order = sorted(range(1, n), key=lambda o: -min(o, n - o))
    for o in order:
        zz = lax.rem(z + o, n)
        greet((row, zz, c))
    greet((row, z, other))

    @pl.when(edge)
    def _():
        def one(i, carry):
            rr = lax.rem(row + i, nrow)
            greet((rr, z, c))
            greet((rr, z, other))
            return carry

        lax.fori_loop(1, nrow, one, 0)

    @pl.when(jnp.logical_not(edge))
    def _():
        for rr in (0, nrow - 1):
            greet((rr, z, c))
            greet((rr, z, other))

    for d in local:
        d.wait()

    def spread(rows_of, target, a, dp):
        turned = rows_of.T
        for s in range(tiles):
            at = pl.multiple_of(dp * width + s * LANES, LANES)
            target[a, pl.ds(at, LANES), :] = jnp.broadcast_to(turned[:, s : s + 1], (LANES, LANES))

    for a in range(2):
        line = edges[a].astype(jnp.float32)
        line = line[7:8] if a == 0 else line[0:1]
        for s in range(tiles):
            edge_row[a, s : s + 1, :] = line[:, s * LANES : (s + 1) * LANES]
    for a in range(2):
        spread(tab[c, z, a], specb, a, c)

    pl.semaphore_wait(barrier, n + jnp.where(edge, 2 * (nrow - 1), 4))

    for o in order:
        where = (row, lax.rem(z + o, n), c)
        for ref, sem in ((tab.at[c, z], tab_sem), (want.at[z], want_sem), (frac.at[z], frac_sem)):
            copy_out(ref, ref, sem.at[0], sem.at[1], where).start()

    def seam_copy(a, i, where_c):
        return copy_out(
            edge_row.at[a],
            seam.at[c, a],
            seam_send,
            seam_recv.at[c, a],
            (lax.rem(row + i, nrow), z, where_c),
        )

    for flag, a in ((last, 0), (first, 1)):

        @pl.when(flag)
        def _(a=a):
            def one(i, carry):
                seam_copy(a, i, 0).start()
                seam_copy(a, i, 1).start()
                return carry

            pltpu.make_async_copy(edge_row.at[a], seam.at[c, a], seam_recv.at[c, a]).start()
            seam_copy(a, 0, other).start()
            lax.fori_loop(1, nrow, one, 0)

    near_copy = copy_out(tab.at[c, z], near, tab_sem.at[4], tab_sem.at[5], (row, z, other))
    near_copy.start()

    a_swap = [
        copy_out(halves.at[a], afull.at[a, :, own], a_sem.at[1 + a], a_sem.at[3 + a], (row, z, other))
        for a in range(2)
    ]
    for d in a_swap:
        d.start()

    def arrived(ref, sem):
        pltpu.make_async_copy(ref, ref, sem).wait()

    near_copy.wait_recv()
    for a in range(2):
        spread(near[a], specb, a, other)

    others = pl.ds(0, n - 1)
    arrived(tab.at[c, others], tab_sem.at[1])
    tab_swap = copy_out(tab.at[c], tab.at[c], tab_sem.at[2], tab_sem.at[3], (row, z, other))
    tab_swap.start()
    pairs = [(dp, a) for dp in range(2) for a in range(2)]
    for dp, a in pairs:
        arrived(seam.at[dp, a], seam_recv.at[dp, a])
    for dp, a in pairs:
        spread(seam[dp, a], seamb, a, dp)
    arrived(want.at[others], want_sem.at[1])
    arrived(frac.at[others], frac_sem.at[1])
    arrived(tab.at[other], tab_sem.at[3])

    table = (tab[...].reshape(4 * n * tiles, LANES) * 0.25).T
    hi = table.astype(jnp.bfloat16)
    rest = table - hi.astype(jnp.float32)
    mid = rest.astype(jnp.bfloat16)
    low = (rest - mid.astype(jnp.float32)).astype(jnp.bfloat16)
    tcat[0:LANES] = hi
    tcat[LANES : 2 * LANES] = mid
    tcat[2 * LANES : 3 * LANES] = low

    def pick(position):
        h = lax.shift_right_logical(position, 1)
        a = position & 1
        g = lax.shift_right_logical(h, log2(width))
        s = lax.shift_right_logical(h, log2(LANES)) & (tiles - 1)
        entry = (((g & 1) * n + lax.shift_right_logical(g, 1)) * 2 + a) * tiles + s
        lane = h & (LANES - 1)
        hit = lax.broadcasted_iota(jnp.int32, (tcat.shape[1], cols), 0) == entry
        onehot = jnp.where(hit, 1.0, 0.0).astype(jnp.bfloat16)
        found = jnp.dot(tcat[...], onehot, preferred_element_type=jnp.float32)
        value = (found[0:LANES] + found[LANES : 2 * LANES]) + found[2 * LANES : 3 * LANES]
        here = lax.broadcasted_iota(jnp.int32, (LANES, cols), 0) == lane
        return jnp.sum(jnp.where(here, value, 0.0), axis=0, keepdims=True) * 4.0

    def roots(d):
        def line(ref):
            block = ref[d]
            return jnp.concatenate([block[b : b + 1] for b in range(kblocks)], axis=1)

        position = line(want)
        lower = pick(position)
        upper = pick(position + 1)
        return lower, line(frac) * (upper - lower)

    def at_offset(off):
        return lax.rem(z + off + n, n)

    def ssq_copy(off):
        return copy_out(
            ssq_s.at[lax.rem(off + n, n)], ssq_r.at[z], ssq_sem.at[0], ssq_sem.at[1], (row, at_offset(off), c)
        )

    step_rows = 64

    def cauchy(a, lower, scaled, carry):
        def one(t, carry):
            at = pl.ds(t * step_rows, step_rows)
            value = specb[a, at, :]
            weight = seamb[a, at, :]
            sums = []
            for b in range(kblocks):
                lanes = slice(b * LANES, (b + 1) * LANES)
                term = weight / ((value - lower[:, lanes]) - scaled[:, lanes])
                ct[at, lanes] = term.astype(jnp.bfloat16)
                squares = (term * term).reshape(step_rows // 8, 8, LANES)
                sums.append(carry[b] + jnp.sum(squares, axis=0))
            return tuple(sums)

        for t in range(2 * width // step_rows):
            carry = one(t, carry)
        return carry

    def product(slot, a):
        part[slot, a] = jnp.dot(afull[a], ct[...], preferred_element_type=jnp.float32)

    steps = n - 1
    m = n // 2

    def ring_copy(j, way, a):
        step = 1 if way == 0 else n - 1
        return copy_out(
            sbuf.at[j, way, a],
            rbuf.at[j, way, a],
            ring_send.at[way, a],
            ring_recv.at[j, way, a],
            (row, lax.rem(z + step, n), c),
        )

    def mine(j, way, a):
        off = m - lax.div(j + 1, 2)
        slot = off if way == 0 else lax.rem(n - off, n)
        start = pl.multiple_of(lax.rem(j + way, 2) * half, half)
        return part[slot, a, pl.ds(start, half), :]

    def launch(j, way, a):
        sbuf[j, way, a] = mine(j, way, a).astype(jnp.bfloat16)
        ring_copy(j, way, a).start()

    def relay(j, way, a):
        ring_copy(j - 2, way, a).wait_recv()
        total = mine(j, way, a) + rbuf[j - 2, way, a].astype(jnp.float32)
        sbuf[j, way, a] = total.astype(jnp.bfloat16)
        ring_copy(j, way, a).start()

    def stage(i, carry):
        odd = lax.rem(i, 2) == 1
        off = jnp.where(odd, m - lax.div(i + 1, 2), lax.div(i, 2) - m)
        slot = lax.rem(off + n, n)
        lower, scaled = roots(at_offset(off))

        def one(a, sums):
            sums = cauchy(a, lower, scaled, sums)
            product(slot, a)
            for way in range(2):

                @pl.when(jnp.logical_or(i == 0, i == way + 1))
                def _(way=way):
                    launch(jnp.minimum(i, 1), way, a)

            return sums

        zeros = tuple(jnp.zeros((8, LANES), jnp.float32) for _ in range(kblocks))
        sums = lax.fori_loop(0, 2, one, zeros)
        for b in range(kblocks):
            ssq_s[slot, b : b + 1, :] = jnp.sum(sums[b], axis=0, keepdims=True)

        @pl.when(i >= 3)
        def _():
            def each(a, carry):
                for way in range(2):
                    relay(i - 1, way, a)
                return carry

            lax.fori_loop(0, 2, each, 0)

        @pl.when(i < n - 1)
        def _():
            ssq_copy(off).start()

        return carry

    a_local.wait()
    for d in a_swap:
        d.wait_recv()
    lax.fori_loop(0, n, stage, 0)

    for ref, sem in ((tab.at[c, others], tab_sem), (want.at[others], want_sem), (frac.at[others], frac_sem)):
        arrived(ref, sem.at[0])
    arrived(ssq_s.at[others], ssq_sem.at[0])
    tab_swap.wait_send()
    for d in a_swap:
        d.wait_send()
    near_copy.wait_send()
    for flag in (last, first):

        @pl.when(flag)
        def _():
            arrived(specb.at[0, pl.ds(0, (2 * nrow - 1) * tiles), :], seam_send)

    arrived(ssq_r.at[others], ssq_sem.at[1])
    total = ssq_s[0]
    for o in range(1, n):
        total = total + ssq_r[lax.rem(z + o, n)]
    norm = jnp.sqrt(total)
    norm = jnp.concatenate([norm[b : b + 1] for b in range(kblocks)], axis=1)
    inverse = 1.0 / norm

    def landed(j, way, a):
        ring_copy(j, way, a).wait_recv()
        hh = (j + way) % 2
        return slice(hh * half, (hh + 1) * half), rbuf[j, way, a].astype(jnp.float32)

    for a in range(2):
        for way in range(2):
            at, value = landed(steps - 2, way, a)
            part[0, a, at, :] += value
    for a in range(2):
        for way in range(2):
            at, value = landed(steps - 1, way, a)
            out[a, at, :] = (part[0, a, at, :] + value) * inverse

    for way in range(2):
        for a in range(2):
            arrived(sbuf.at[:, way, a], ring_send.at[way, a])


def merge(nrow, n, halves, spectrum, wanted, fraction):
    rows, width = halves.shape[1:]
    tiles = width // LANES
    cols = wanted.shape[0] // 2
    kblocks = cols // LANES
    spectrum = spectrum.reshape(2, tiles, LANES).transpose(1, 0, 2)
    operands = (halves, spectrum, wanted.reshape(2, kblocks, LANES), fraction.reshape(2, kblocks, LANES))
    half = rows // 2
    steps = n - 1
    bf16, f32 = jnp.bfloat16, jnp.float32
    return pl.pallas_call(
        functools.partial(kernel, nrow, n),
        out_shape=jax.ShapeDtypeStruct((2, rows, cols), f32),
        in_specs=[pl.BlockSpec(memory_space=pltpu.HBM)] * 4,
        out_specs=pl.BlockSpec(memory_space=pltpu.VMEM),
        scratch_shapes=[
            pltpu.VMEM((2, rows, 2 * width), bf16),
            pltpu.VMEM((2, 8, width), bf16),
            pltpu.VMEM((2, tiles, LANES), f32),
            pltpu.VMEM((2, n, 2, tiles, LANES), f32),
            pltpu.VMEM((2, tiles, LANES), f32),
            pltpu.VMEM((n, kblocks, LANES), jnp.int32),
            pltpu.VMEM((n, kblocks, LANES), f32),
            pltpu.VMEM((2, 2, tiles, LANES), f32),
            pltpu.VMEM((2, 2 * width, LANES), f32),
            pltpu.VMEM((2, 2 * width, LANES), f32),
            pltpu.VMEM((3 * LANES, 4 * n * tiles), bf16),
            pltpu.VMEM((2 * width, cols), bf16),
            pltpu.VMEM((n, 2, rows, cols), f32),
            pltpu.VMEM((steps, 2, 2, half, cols), bf16),
            pltpu.VMEM((steps, 2, 2, half, cols), bf16),
            pltpu.VMEM((n, kblocks, LANES), f32),
            pltpu.VMEM((n, kblocks, LANES), f32),
            pltpu.SemaphoreType.DMA((5,)),
            pltpu.SemaphoreType.DMA((6,)),
            pltpu.SemaphoreType.DMA((6,)),
            pltpu.SemaphoreType.DMA((2,)),
            pltpu.SemaphoreType.DMA((2,)),
            pltpu.SemaphoreType.DMA,
            pltpu.SemaphoreType.DMA((2, 2)),
            pltpu.SemaphoreType.DMA((2, 2)),
            pltpu.SemaphoreType.DMA((steps, 2, 2)),
            pltpu.SemaphoreType.DMA((2,)),
        ],
        compiler_params=pltpu.CompilerParams(
            collective_id=0, has_side_effects=True, vmem_limit_bytes=48 * 1024 * 1024
        ),
        name="merge",
    )(*[pltpu.with_memory_space_constraint(x, pltpu.HBM) for x in operands])


def solution(mesh):
    body = functools.partial(merge, mesh.shape["row"], mesh.shape["col"])
    in_specs = (P(None, "row", ("col", "depth")), P(None, ("col", "depth")), P("col"), P("col"))
    out_specs = P(None, "row", ("col", "depth"))
    return jax.shard_map(body, mesh=mesh, in_specs=in_specs, out_specs=out_specs, check_vma=False)
```

```python
import functools

import jax
import jax.numpy as jnp
from jax import lax
from jax.experimental import pallas as pl
from jax.experimental.pallas import tpu as pltpu
from jax.sharding import PartitionSpec as P

MESH = pl.DeviceIdType.MESH
LANES = 128


def log2(x):
    return x.bit_length() - 1


def kernel(
    nrow,
    n,
    halves,
    spectrum,
    wanted,
    fraction,
    out,
    afull,
    edges,
    edge_row,
    tab,
    near,
    want,
    frac,
    seam,
    specb,
    seamb,
    tcat,
    ct,
    part,
    sbuf,
    rbuf,
    ssq_s,
    ssq_r,
    a_sem,
    local_sem,
    tab_sem,
    want_sem,
    frac_sem,
    seam_send,
    seam_recv,
    ring_send,
    ring_recv,
    ssq_sem,
):
    row, z, c = lax.axis_index("row"), lax.axis_index("col"), lax.axis_index("depth")
    rows, width = halves.shape[1], halves.shape[2]
    tiles = width // LANES
    cols = out.shape[2]
    kblocks = cols // LANES
    half = rows // 2
    other = 1 - c
    first, last = row == 0, row == nrow - 1
    edge = jnp.logical_or(first, last)

    def copy_out(src, dst, send, recv, where):
        return pltpu.make_async_remote_copy(
            src_ref=src, dst_ref=dst, send_sem=send, recv_sem=recv, device_id=where, device_id_type=MESH
        )

    own = pl.ds(pl.multiple_of(c * width, width), width)
    sources = [
        (spectrum.at[:, 0], tab.at[c, z, 0]),
        (spectrum.at[:, 1], tab.at[c, z, 1]),
        (wanted.at[c], want.at[z]),
        (fraction.at[c], frac.at[z]),
        (halves.at[0, pl.ds(rows - 8, 8)], edges.at[0]),
        (halves.at[1, pl.ds(0, 8)], edges.at[1]),
    ]
    local = [pltpu.make_async_copy(src, dst, local_sem.at[k]) for k, (src, dst) in enumerate(sources)]
    for d in local:
        d.start()
    a_local = pltpu.make_async_copy(halves, afull.at[:, :, own], a_sem.at[0])
    a_local.start()

    barrier = pltpu.get_barrier_semaphore()

    def greet(where):
        pl.semaphore_signal(barrier, inc=1, device_id=where, device_id_type=MESH)

    order = sorted(range(1, n), key=lambda o: -min(o, n - o))
    for o in order:
        zz = lax.rem(z + o, n)
        greet((row, zz, c))
    greet((row, z, other))

    @pl.when(edge)
    def _():
        def one(i, carry):
            rr = lax.rem(row + i, nrow)
            greet((rr, z, c))
            greet((rr, z, other))
            return carry

        lax.fori_loop(1, nrow, one, 0)

    @pl.when(jnp.logical_not(edge))
    def _():
        for rr in (0, nrow - 1):
            greet((rr, z, c))
            greet((rr, z, other))

    for d in local:
        d.wait()

    def spread(rows_of, target, a, dp):
        turned = rows_of.T
        for s in range(tiles):
            at = pl.multiple_of(dp * width + s * LANES, LANES)
            target[a, pl.ds(at, LANES), :] = jnp.broadcast_to(turned[:, s : s + 1], (LANES, LANES))

    for a in range(2):
        line = edges[a].astype(jnp.float32)
        line = line[7:8] if a == 0 else line[0:1]
        for s in range(tiles):
            edge_row[a, s : s + 1, :] = line[:, s * LANES : (s + 1) * LANES]
    for a in range(2):
        spread(tab[c, z, a], specb, a, c)

    pl.semaphore_wait(barrier, n + jnp.where(edge, 2 * (nrow - 1), 4))

    for o in order:
        where = (row, lax.rem(z + o, n), c)
        for ref, sem in ((tab.at[c, z], tab_sem), (want.at[z], want_sem), (frac.at[z], frac_sem)):
            copy_out(ref, ref, sem.at[0], sem.at[1], where).start()

    def seam_copy(a, i, where_c):
        return copy_out(
            edge_row.at[a],
            seam.at[c, a],
            seam_send,
            seam_recv.at[c, a],
            (lax.rem(row + i, nrow), z, where_c),
        )

    for flag, a in ((last, 0), (first, 1)):

        @pl.when(flag)
        def _(a=a):
            def one(i, carry):
                seam_copy(a, i, 0).start()
                seam_copy(a, i, 1).start()
                return carry

            pltpu.make_async_copy(edge_row.at[a], seam.at[c, a], seam_recv.at[c, a]).start()
            seam_copy(a, 0, other).start()
            lax.fori_loop(1, nrow, one, 0)

    near_copy = copy_out(tab.at[c, z], near, tab_sem.at[4], tab_sem.at[5], (row, z, other))
    near_copy.start()

    a_swap = [
        copy_out(halves.at[a], afull.at[a, :, own], a_sem.at[1 + a], a_sem.at[3 + a], (row, z, other))
        for a in range(2)
    ]
    for d in a_swap:
        d.start()

    def arrived(ref, sem):
        pltpu.make_async_copy(ref, ref, sem).wait()

    near_copy.wait_recv()

    def onward(o):
        return copy_out(near, tab.at[0, z], tab_sem.at[6], tab_sem.at[2], (row, lax.rem(z + o, n), c))

    @pl.when(c == 1)
    def _():
        for o in order:
            onward(o).start()

    for a in range(2):
        spread(near[a], specb, a, other)

    others = pl.ds(0, n - 1)
    arrived(tab.at[c, others], tab_sem.at[1])
    tab_swap = copy_out(tab.at[1], tab.at[1], tab_sem.at[3], tab_sem.at[2], (row, z, 0))

    @pl.when(c == 1)
    def _():
        tab_swap.start()
        tab[0, z] = near[...]

    pairs = [(dp, a) for dp in range(2) for a in range(2)]
    for dp, a in pairs:
        arrived(seam.at[dp, a], seam_recv.at[dp, a])
    for dp in range(2):
        spread(seam[dp, 0], seamb, 0, dp)
    arrived(want.at[others], want_sem.at[1])
    arrived(frac.at[others], frac_sem.at[1])

    @pl.when(c == 0)
    def _():
        arrived(tab.at[1], tab_sem.at[2])

    @pl.when(c == 1)
    def _():
        arrived(tab.at[0, others], tab_sem.at[2])


    table = (tab[...].reshape(4 * n * tiles, LANES) * 0.25).T
    hi = table.astype(jnp.bfloat16)
    rest = table - hi.astype(jnp.float32)
    mid = rest.astype(jnp.bfloat16)
    low = (rest - mid.astype(jnp.float32)).astype(jnp.bfloat16)
    tcat[0:LANES] = hi
    tcat[LANES : 2 * LANES] = mid
    tcat[2 * LANES : 3 * LANES] = low

    def pick(position):
        h = lax.shift_right_logical(position, 1)
        a = position & 1
        g = lax.shift_right_logical(h, log2(width))
        s = lax.shift_right_logical(h, log2(LANES)) & (tiles - 1)
        entry = (((g & 1) * n + lax.shift_right_logical(g, 1)) * 2 + a) * tiles + s
        lane = h & (LANES - 1)
        hit = lax.broadcasted_iota(jnp.int32, (tcat.shape[1], cols), 0) == entry
        onehot = jnp.where(hit, 1.0, 0.0).astype(jnp.bfloat16)
        found = jnp.dot(tcat[...], onehot, preferred_element_type=jnp.float32)
        value = (found[0:LANES] + found[LANES : 2 * LANES]) + found[2 * LANES : 3 * LANES]
        here = lax.broadcasted_iota(jnp.int32, (LANES, cols), 0) == lane
        return jnp.sum(jnp.where(here, value, 0.0), axis=0, keepdims=True) * 4.0

    def roots(d):
        def line(ref):
            block = ref[d]
            return jnp.concatenate([block[b : b + 1] for b in range(kblocks)], axis=1)

        position = line(want)
        lower = pick(position)
        upper = pick(position + 1)
        return lower, line(frac) * (upper - lower)

    def at_offset(off):
        return lax.rem(z + off + n, n)

    def ssq_copy(off):
        return copy_out(
            ssq_s.at[lax.rem(off + n, n)], ssq_r.at[z], ssq_sem.at[0], ssq_sem.at[1], (row, at_offset(off), c)
        )

    step_rows = 64

    def cauchy(a, lower, scaled, carry):
        def one(t, carry):
            at = pl.ds(t * step_rows, step_rows)
            value = specb[a, at, :]
            weight = seamb[a, at, :]
            sums = []
            for b in range(kblocks):
                lanes = slice(b * LANES, (b + 1) * LANES)
                term = weight / ((value - lower[:, lanes]) - scaled[:, lanes])
                ct[at, lanes] = term.astype(jnp.bfloat16)
                squares = (term * term).reshape(step_rows // 8, 8, LANES)
                sums.append(carry[b] + jnp.sum(squares, axis=0))
            return tuple(sums)

        for t in range(2 * width // step_rows):
            carry = one(t, carry)
        return carry

    def product(slot, a):
        part[slot, a] = jnp.dot(afull[a], ct[...], preferred_element_type=jnp.float32)

    steps = n - 1
    m = n // 2

    def ring_copy(j, way, a):
        step = 1 if way == 0 else n - 1
        return copy_out(
            sbuf.at[j, way, a],
            rbuf.at[j, way, a],
            ring_send.at[way, a],
            ring_recv.at[j, way, a],
            (row, lax.rem(z + step, n), c),
        )

    def mine(j, way, a):
        off = m - lax.div(j + 1, 2)
        slot = off if way == 0 else lax.rem(n - off, n)
        start = pl.multiple_of(lax.rem(j + way, 2) * half, half)
        return part[slot, a, pl.ds(start, half), :]

    def launch(j, way, a):
        sbuf[j, way, a] = mine(j, way, a).astype(jnp.bfloat16)
        ring_copy(j, way, a).start()

    def relay(j, way, a):
        ring_copy(j - 2, way, a).wait_recv()
        total = mine(j, way, a) + rbuf[j - 2, way, a].astype(jnp.float32)
        sbuf[j, way, a] = total.astype(jnp.bfloat16)
        ring_copy(j, way, a).start()

    def stage(i, carry):
        odd = lax.rem(i, 2) == 1
        off = jnp.where(odd, m - lax.div(i + 1, 2), lax.div(i, 2) - m)
        slot = lax.rem(off + n, n)
        lower, scaled = roots(at_offset(off))

        def one(a, sums):
            sums = cauchy(a, lower, scaled, sums)
            product(slot, a)
            for way in range(2):

                @pl.when(jnp.logical_or(i == 0, i == way + 1))
                def _(way=way):
                    launch(jnp.minimum(i, 1), way, a)

            @pl.when(jnp.logical_and(i == 0, a == 0))
            def _():
                for dp in range(2):
                    spread(seam[dp, 1], seamb, 1, dp)

            return sums

        zeros = tuple(jnp.zeros((8, LANES), jnp.float32) for _ in range(kblocks))
        sums = lax.fori_loop(0, 2, one, zeros)
        for b in range(kblocks):
            ssq_s[slot, b : b + 1, :] = jnp.sum(sums[b], axis=0, keepdims=True)

        @pl.when(i >= 3)
        def _():
            def each(a, carry):
                for way in range(2):
                    relay(i - 1, way, a)
                return carry

            lax.fori_loop(0, 2, each, 0)

        @pl.when(i < n - 1)
        def _():
            ssq_copy(off).start()

        return carry

    a_local.wait()
    for d in a_swap:
        d.wait_recv()
    lax.fori_loop(0, n, stage, 0)

    for ref, sem in ((tab.at[c, others], tab_sem), (want.at[others], want_sem), (frac.at[others], frac_sem)):
        arrived(ref, sem.at[0])
    arrived(ssq_s.at[others], ssq_sem.at[0])

    @pl.when(c == 1)
    def _():
        tab_swap.wait_send()
        arrived(tab.at[0, others], tab_sem.at[6])

    for d in a_swap:
        d.wait_send()
    near_copy.wait_send()
    for flag in (last, first):

        @pl.when(flag)
        def _():
            arrived(specb.at[0, pl.ds(0, (2 * nrow - 1) * tiles), :], seam_send)

    arrived(ssq_r.at[others], ssq_sem.at[1])
    total = ssq_s[0]
    for o in range(1, n):
        total = total + ssq_r[lax.rem(z + o, n)]
    norm = jnp.sqrt(total)
    norm = jnp.concatenate([norm[b : b + 1] for b in range(kblocks)], axis=1)
    inverse = 1.0 / norm

    def landed(j, way, a):
        ring_copy(j, way, a).wait_recv()
        hh = (j + way) % 2
        return slice(hh * half, (hh + 1) * half), rbuf[j, way, a].astype(jnp.float32)

    for a in range(2):
        for way in range(2):
            at, value = landed(steps - 2, way, a)
            part[0, a, at, :] += value
    for a in range(2):
        for way in range(2):
            at, value = landed(steps - 1, way, a)
            out[a, at, :] = (part[0, a, at, :] + value) * inverse

    for way in range(2):
        for a in range(2):
            arrived(sbuf.at[:, way, a], ring_send.at[way, a])


def merge(nrow, n, halves, spectrum, wanted, fraction):
    rows, width = halves.shape[1:]
    tiles = width // LANES
    cols = wanted.shape[0] // 2
    kblocks = cols // LANES
    spectrum = spectrum.reshape(2, tiles, LANES).transpose(1, 0, 2)
    operands = (halves, spectrum, wanted.reshape(2, kblocks, LANES), fraction.reshape(2, kblocks, LANES))
    half = rows // 2
    steps = n - 1
    bf16, f32 = jnp.bfloat16, jnp.float32
    return pl.pallas_call(
        functools.partial(kernel, nrow, n),
        out_shape=jax.ShapeDtypeStruct((2, rows, cols), f32),
        in_specs=[pl.BlockSpec(memory_space=pltpu.HBM)] * 4,
        out_specs=pl.BlockSpec(memory_space=pltpu.VMEM),
        scratch_shapes=[
            pltpu.VMEM((2, rows, 2 * width), bf16),
            pltpu.VMEM((2, 8, width), bf16),
            pltpu.VMEM((2, tiles, LANES), f32),
            pltpu.VMEM((2, n, 2, tiles, LANES), f32),
            pltpu.VMEM((2, tiles, LANES), f32),
            pltpu.VMEM((n, kblocks, LANES), jnp.int32),
            pltpu.VMEM((n, kblocks, LANES), f32),
            pltpu.VMEM((2, 2, tiles, LANES), f32),
            pltpu.VMEM((2, 2 * width, LANES), f32),
            pltpu.VMEM((2, 2 * width, LANES), f32),
            pltpu.VMEM((3 * LANES, 4 * n * tiles), bf16),
            pltpu.VMEM((2 * width, cols), bf16),
            pltpu.VMEM((n, 2, rows, cols), f32),
            pltpu.VMEM((steps, 2, 2, half, cols), bf16),
            pltpu.VMEM((steps, 2, 2, half, cols), bf16),
            pltpu.VMEM((n, kblocks, LANES), f32),
            pltpu.VMEM((n, kblocks, LANES), f32),
            pltpu.SemaphoreType.DMA((5,)),
            pltpu.SemaphoreType.DMA((6,)),
            pltpu.SemaphoreType.DMA((7,)),
            pltpu.SemaphoreType.DMA((2,)),
            pltpu.SemaphoreType.DMA((2,)),
            pltpu.SemaphoreType.DMA,
            pltpu.SemaphoreType.DMA((2, 2)),
            pltpu.SemaphoreType.DMA((2, 2)),
            pltpu.SemaphoreType.DMA((steps, 2, 2)),
            pltpu.SemaphoreType.DMA((2,)),
        ],
        compiler_params=pltpu.CompilerParams(
            collective_id=0, has_side_effects=True, vmem_limit_bytes=48 * 1024 * 1024
        ),
        name="merge",
    )(*[pltpu.with_memory_space_constraint(x, pltpu.HBM) for x in operands])


def solution(mesh):
    body = functools.partial(merge, mesh.shape["row"], mesh.shape["col"])
    in_specs = (P(None, "row", ("col", "depth")), P(None, ("col", "depth")), P("col"), P("col"))
    out_specs = P(None, "row", ("col", "depth"))
    return jax.shard_map(body, mesh=mesh, in_specs=in_specs, out_specs=out_specs, check_vma=False)
```

```python
import functools

import jax
import jax.numpy as jnp
from jax import lax
from jax.experimental import pallas as pl
from jax.experimental.pallas import tpu as pltpu
from jax.sharding import PartitionSpec as P

MESH = pl.DeviceIdType.MESH
LANES = 128


def log2(x):
    return x.bit_length() - 1


def kernel(
    nrow,
    n,
    halves,
    spectrum,
    wanted,
    fraction,
    out,
    afull,
    edges,
    edge_row,
    tab,
    near,
    want,
    frac,
    seam,
    specb,
    seamb,
    tcat,
    ct,
    root,
    ssq,
    part,
    sbuf,
    rbuf,
    ssq_s,
    ssq_r,
    a_sem,
    local_sem,
    tab_sem,
    want_sem,
    frac_sem,
    seam_send,
    seam_recv,
    ring_send,
    ring_recv,
    ssq_sem,
):
    row, z, c = lax.axis_index("row"), lax.axis_index("col"), lax.axis_index("depth")
    rows, width = halves.shape[1], halves.shape[2]
    tiles = width // LANES
    cols = out.shape[2]
    kblocks = cols // LANES
    half = rows // 2
    other = 1 - c
    first, last = row == 0, row == nrow - 1
    edge = jnp.logical_or(first, last)

    def copy_out(src, dst, send, recv, where):
        return pltpu.make_async_remote_copy(
            src_ref=src, dst_ref=dst, send_sem=send, recv_sem=recv, device_id=where, device_id_type=MESH
        )

    own = pl.ds(pl.multiple_of(c * width, width), width)
    sources = [
        (spectrum.at[:, 0], tab.at[c, z, 0]),
        (spectrum.at[:, 1], tab.at[c, z, 1]),
        (wanted.at[c], want.at[z]),
        (fraction.at[c], frac.at[z]),
        (halves.at[0, pl.ds(rows - 8, 8)], edges.at[0]),
        (halves.at[1, pl.ds(0, 8)], edges.at[1]),
    ]
    local = [pltpu.make_async_copy(src, dst, local_sem.at[k]) for k, (src, dst) in enumerate(sources)]
    for d in local:
        d.start()
    a_local = pltpu.make_async_copy(halves, afull.at[:, :, own], a_sem.at[0])
    a_local.start()

    barrier = pltpu.get_barrier_semaphore()

    def greet(where):
        pl.semaphore_signal(barrier, inc=1, device_id=where, device_id_type=MESH)

    order = sorted(range(1, n), key=lambda o: -min(o, n - o))
    for o in order:
        zz = lax.rem(z + o, n)
        greet((row, zz, c))
    greet((row, z, other))

    @pl.when(edge)
    def _():
        def one(i, carry):
            rr = lax.rem(row + i, nrow)
            greet((rr, z, c))
            greet((rr, z, other))
            return carry

        lax.fori_loop(1, nrow, one, 0)

    @pl.when(jnp.logical_not(edge))
    def _():
        for rr in (0, nrow - 1):
            greet((rr, z, c))
            greet((rr, z, other))

    for d in local:
        d.wait()

    def spread(rows_of, target, a, dp):
        turned = rows_of.T
        for s in range(tiles):
            at = pl.multiple_of(dp * width + s * LANES, LANES)
            target[a, pl.ds(at, LANES), :] = jnp.broadcast_to(turned[:, s : s + 1], (LANES, LANES))

    for a in range(2):
        line = edges[a].astype(jnp.float32)
        line = line[7:8] if a == 0 else line[0:1]
        for s in range(tiles):
            edge_row[a, s : s + 1, :] = line[:, s * LANES : (s + 1) * LANES]
    for a in range(2):
        spread(tab[c, z, a], specb, a, c)

    pl.semaphore_wait(barrier, n + jnp.where(edge, 2 * (nrow - 1), 4))

    for o in order:
        where = (row, lax.rem(z + o, n), c)
        for ref, sem in ((tab.at[c, z], tab_sem), (want.at[z], want_sem), (frac.at[z], frac_sem)):
            copy_out(ref, ref, sem.at[0], sem.at[1], where).start()

    def seam_copy(a, i, where_c):
        return copy_out(
            edge_row.at[a],
            seam.at[c, a],
            seam_send,
            seam_recv.at[c, a],
            (lax.rem(row + i, nrow), z, where_c),
        )

    for flag, a in ((last, 0), (first, 1)):

        @pl.when(flag)
        def _(a=a):
            def one(i, carry):
                seam_copy(a, i, 0).start()
                seam_copy(a, i, 1).start()
                return carry

            pltpu.make_async_copy(edge_row.at[a], seam.at[c, a], seam_recv.at[c, a]).start()
            seam_copy(a, 0, other).start()
            lax.fori_loop(1, nrow, one, 0)

    near_copy = copy_out(tab.at[c, z], near, tab_sem.at[4], tab_sem.at[5], (row, z, other))
    near_copy.start()

    a_swap = [
        copy_out(halves.at[a], afull.at[a, :, own], a_sem.at[1 + a], a_sem.at[3 + a], (row, z, other))
        for a in range(2)
    ]
    for d in a_swap:
        d.start()

    def arrived(ref, sem):
        pltpu.make_async_copy(ref, ref, sem).wait()

    near_copy.wait_recv()

    def onward(o):
        return copy_out(near, tab.at[0, z], tab_sem.at[6], tab_sem.at[2], (row, lax.rem(z + o, n), c))

    @pl.when(c == 1)
    def _():
        for o in order:
            onward(o).start()

    for a in range(2):
        spread(near[a], specb, a, other)

    others = pl.ds(0, n - 1)
    arrived(tab.at[c, others], tab_sem.at[1])
    tab_swap = copy_out(tab.at[1], tab.at[1], tab_sem.at[3], tab_sem.at[2], (row, z, 0))

    @pl.when(c == 1)
    def _():
        tab_swap.start()
        tab[0, z] = near[...]

    pairs = [(dp, a) for dp in range(2) for a in range(2)]
    for dp, a in pairs:
        arrived(seam.at[dp, a], seam_recv.at[dp, a])
    for dp in range(2):
        spread(seam[dp, 0], seamb, 0, dp)
    arrived(want.at[others], want_sem.at[1])
    arrived(frac.at[others], frac_sem.at[1])

    @pl.when(c == 0)
    def _():
        arrived(tab.at[1], tab_sem.at[2])

    @pl.when(c == 1)
    def _():
        arrived(tab.at[0, others], tab_sem.at[2])


    table = (tab[...].reshape(4 * n * tiles, LANES) * 0.25).T
    hi = table.astype(jnp.bfloat16)
    rest = table - hi.astype(jnp.float32)
    mid = rest.astype(jnp.bfloat16)
    low = (rest - mid.astype(jnp.float32)).astype(jnp.bfloat16)
    tcat[0:LANES] = hi
    tcat[LANES : 2 * LANES] = mid
    tcat[2 * LANES : 3 * LANES] = low

    def pick(position):
        h = lax.shift_right_logical(position, 1)
        a = position & 1
        g = lax.shift_right_logical(h, log2(width))
        s = lax.shift_right_logical(h, log2(LANES)) & (tiles - 1)
        entry = (((g & 1) * n + lax.shift_right_logical(g, 1)) * 2 + a) * tiles + s
        lane = h & (LANES - 1)
        hit = lax.broadcasted_iota(jnp.int32, (tcat.shape[1], cols), 0) == entry
        onehot = jnp.where(hit, 1.0, 0.0).astype(jnp.bfloat16)
        found = jnp.dot(tcat[...], onehot, preferred_element_type=jnp.float32)
        value = (found[0:LANES] + found[LANES : 2 * LANES]) + found[2 * LANES : 3 * LANES]
        here = lax.broadcasted_iota(jnp.int32, (LANES, cols), 0) == lane
        return jnp.sum(jnp.where(here, value, 0.0), axis=0, keepdims=True) * 4.0

    def roots(d):
        def line(ref):
            block = ref[d]
            return jnp.concatenate([block[b : b + 1] for b in range(kblocks)], axis=1)

        position = line(want)
        lower = pick(position)
        upper = pick(position + 1)
        return lower, line(frac) * (upper - lower)

    def at_offset(off):
        return lax.rem(z + off + n, n)

    def ssq_copy(off):
        return copy_out(
            ssq_s.at[lax.rem(off + n, n)], ssq_r.at[z], ssq_sem.at[0], ssq_sem.at[1], (row, at_offset(off), c)
        )

    step_rows = 64

    def cauchy(a, lower, scaled, carry):
        def one(t, carry):
            at = pl.ds(t * step_rows, step_rows)
            value = specb[a, at, :]
            weight = seamb[a, at, :]
            sums = []
            for b in range(kblocks):
                lanes = slice(b * LANES, (b + 1) * LANES)
                term = weight / ((value - lower[:, lanes]) - scaled[:, lanes])
                ct[at, lanes] = term.astype(jnp.bfloat16)
                squares = (term * term).reshape(step_rows // 8, 8, LANES)
                sums.append(carry[b] + jnp.sum(squares, axis=0))
            return tuple(sums)

        for t in range(2 * width // step_rows):
            carry = one(t, carry)
        return carry

    def product(slot, a):
        part[slot, a] = jnp.dot(afull[a], ct[...], preferred_element_type=jnp.float32)

    steps = n - 1
    m = n // 2

    def ring_copy(j, way, a):
        step = 1 if way == 0 else n - 1
        return copy_out(
            sbuf.at[j, way, a],
            rbuf.at[j, way, a],
            ring_send.at[way, a],
            ring_recv.at[j, way, a],
            (row, lax.rem(z + step, n), c),
        )

    def mine(j, way, a):
        off = m - lax.div(j + 1, 2)
        slot = off if way == 0 else lax.rem(n - off, n)
        start = pl.multiple_of(lax.rem(j + way, 2) * half, half)
        return part[slot, a, pl.ds(start, half), :]

    def launch(j, way, a):
        sbuf[j, way, a] = mine(j, way, a).astype(jnp.bfloat16)
        ring_copy(j, way, a).start()

    def relay(j, way, a):
        ring_copy(j - 2, way, a).wait_recv()
        total = mine(j, way, a) + rbuf[j - 2, way, a].astype(jnp.float32)
        sbuf[j, way, a] = total.astype(jnp.bfloat16)
        ring_copy(j, way, a).start()

    def unit(u, carry):
        ends = jnp.logical_or(u < 2, u >= 2 * n - 2)
        pair = jnp.where(ends, jnp.where(u < 2, 0, m), lax.div(u + 2, 4))
        turn = jnp.where(ends, 0, lax.rem(u, 2))
        a = jnp.where(ends, lax.rem(u, 2), lax.div(lax.rem(u + 2, 4), 2))
        off = jnp.where(turn == 0, m - pair, pair - m)
        slot = lax.rem(off + n, n)

        @pl.when(a == 0)
        def _():
            lower, scaled = roots(at_offset(off))
            root[turn, 0] = lower
            root[turn, 1] = scaled
            ssq[turn] = jnp.zeros(ssq.shape[1:], jnp.float32)

        sums = cauchy(a, root[turn, 0], root[turn, 1], tuple(ssq[turn, b] for b in range(kblocks)))
        product(slot, a)
        for b in range(kblocks):
            ssq[turn, b] = sums[b]

        @pl.when(jnp.logical_and(c == 0, u == 2))
        def _():
            def both(k, carry):
                for way in range(2):
                    launch(0, way, k)
                return carry

            lax.fori_loop(0, 2, both, 0)

        for way in range(2):
            first = jnp.logical_or(
                jnp.logical_and(u < 2, c == 1), jnp.logical_and(pair == 1, turn == way)
            )

            @pl.when(first)
            def _(way=way):
                launch(jnp.minimum(pair, 1), way, a)

        @pl.when(u == 0)
        def _():
            for dp in range(2):
                spread(seam[dp, 1], seamb, 1, dp)

        @pl.when(a == 1)
        def _():
            for b in range(kblocks):
                ssq_s[slot, b : b + 1, :] = jnp.sum(ssq[turn, b], axis=0, keepdims=True)

            @pl.when(u < 2 * n - 1)
            def _():
                ssq_copy(off).start()

        @pl.when(jnp.logical_and(lax.rem(u, 4) == 1, jnp.logical_and(u >= 5, u < 2 * n - 2)))
        def _():
            relays(lax.div(u + 3, 4))

        return carry

    def relays(j):
        def each(a, carry):
            for way in range(2):
                relay(j, way, a)
            return carry

        lax.fori_loop(0, 2, each, 0)

    a_local.wait()
    for d in a_swap:
        d.wait_recv()
    lax.fori_loop(0, 2 * n, unit, 0)

    def rest(j, carry):
        relays(j)
        return carry

    lax.fori_loop(m + 1, steps, rest, 0)

    for ref, sem in ((tab.at[c, others], tab_sem), (want.at[others], want_sem), (frac.at[others], frac_sem)):
        arrived(ref, sem.at[0])
    arrived(ssq_s.at[others], ssq_sem.at[0])

    @pl.when(c == 1)
    def _():
        tab_swap.wait_send()
        arrived(tab.at[0, others], tab_sem.at[6])

    for d in a_swap:
        d.wait_send()
    near_copy.wait_send()
    for flag in (last, first):

        @pl.when(flag)
        def _():
            arrived(specb.at[0, pl.ds(0, (2 * nrow - 1) * tiles), :], seam_send)

    arrived(ssq_r.at[others], ssq_sem.at[1])
    total = ssq_s[0]
    for o in range(1, n):
        total = total + ssq_r[lax.rem(z + o, n)]
    norm = jnp.sqrt(total)
    norm = jnp.concatenate([norm[b : b + 1] for b in range(kblocks)], axis=1)
    inverse = 1.0 / norm

    def landed(j, way, a):
        ring_copy(j, way, a).wait_recv()
        hh = (j + way) % 2
        return slice(hh * half, (hh + 1) * half), rbuf[j, way, a].astype(jnp.float32)

    for a in range(2):
        for way in range(2):
            at, value = landed(steps - 2, way, a)
            part[0, a, at, :] += value
    for a in range(2):
        for way in range(2):
            at, value = landed(steps - 1, way, a)
            out[a, at, :] = (part[0, a, at, :] + value) * inverse

    for way in range(2):
        for a in range(2):
            arrived(sbuf.at[:, way, a], ring_send.at[way, a])


def merge(nrow, n, halves, spectrum, wanted, fraction):
    rows, width = halves.shape[1:]
    tiles = width // LANES
    cols = wanted.shape[0] // 2
    kblocks = cols // LANES
    spectrum = spectrum.reshape(2, tiles, LANES).transpose(1, 0, 2)
    operands = (halves, spectrum, wanted.reshape(2, kblocks, LANES), fraction.reshape(2, kblocks, LANES))
    half = rows // 2
    steps = n - 1
    bf16, f32 = jnp.bfloat16, jnp.float32
    return pl.pallas_call(
        functools.partial(kernel, nrow, n),
        out_shape=jax.ShapeDtypeStruct((2, rows, cols), f32),
        in_specs=[pl.BlockSpec(memory_space=pltpu.HBM)] * 4,
        out_specs=pl.BlockSpec(memory_space=pltpu.VMEM),
        scratch_shapes=[
            pltpu.VMEM((2, rows, 2 * width), bf16),
            pltpu.VMEM((2, 8, width), bf16),
            pltpu.VMEM((2, tiles, LANES), f32),
            pltpu.VMEM((2, n, 2, tiles, LANES), f32),
            pltpu.VMEM((2, tiles, LANES), f32),
            pltpu.VMEM((n, kblocks, LANES), jnp.int32),
            pltpu.VMEM((n, kblocks, LANES), f32),
            pltpu.VMEM((2, 2, tiles, LANES), f32),
            pltpu.VMEM((2, 2 * width, LANES), f32),
            pltpu.VMEM((2, 2 * width, LANES), f32),
            pltpu.VMEM((3 * LANES, 4 * n * tiles), bf16),
            pltpu.VMEM((2 * width, cols), bf16),
            pltpu.VMEM((2, 2, 1, cols), f32),
            pltpu.VMEM((2, kblocks, 8, LANES), f32),
            pltpu.VMEM((n, 2, rows, cols), f32),
            pltpu.VMEM((steps, 2, 2, half, cols), bf16),
            pltpu.VMEM((steps, 2, 2, half, cols), bf16),
            pltpu.VMEM((n, kblocks, LANES), f32),
            pltpu.VMEM((n, kblocks, LANES), f32),
            pltpu.SemaphoreType.DMA((5,)),
            pltpu.SemaphoreType.DMA((6,)),
            pltpu.SemaphoreType.DMA((7,)),
            pltpu.SemaphoreType.DMA((2,)),
            pltpu.SemaphoreType.DMA((2,)),
            pltpu.SemaphoreType.DMA,
            pltpu.SemaphoreType.DMA((2, 2)),
            pltpu.SemaphoreType.DMA((2, 2)),
            pltpu.SemaphoreType.DMA((steps, 2, 2)),
            pltpu.SemaphoreType.DMA((2,)),
        ],
        compiler_params=pltpu.CompilerParams(
            collective_id=0, has_side_effects=True, vmem_limit_bytes=48 * 1024 * 1024
        ),
        name="merge",
    )(*[pltpu.with_memory_space_constraint(x, pltpu.HBM) for x in operands])


def solution(mesh):
    body = functools.partial(merge, mesh.shape["row"], mesh.shape["col"])
    in_specs = (P(None, "row", ("col", "depth")), P(None, ("col", "depth")), P("col"), P("col"))
    out_specs = P(None, "row", ("col", "depth"))
    return jax.shard_map(body, mesh=mesh, in_specs=in_specs, out_specs=out_specs, check_vma=False)
```

```python
import functools

import jax
import jax.numpy as jnp
from jax import lax
from jax.experimental import pallas as pl
from jax.experimental.pallas import tpu as pltpu
from jax.sharding import PartitionSpec as P

MESH = pl.DeviceIdType.MESH
LANES = 128


def log2(x):
    return x.bit_length() - 1


def kernel(
    nrow,
    n,
    halves,
    spectrum,
    wanted,
    fraction,
    out,
    afull,
    edges,
    edge_row,
    tab,
    near,
    want,
    frac,
    seam,
    specb,
    seamb,
    tcat,
    ct,
    root,
    ssq,
    part,
    sbuf,
    rbuf,
    ssq_s,
    ssq_r,
    a_sem,
    local_sem,
    tab_sem,
    want_sem,
    frac_sem,
    seam_send,
    seam_recv,
    ring_send,
    ring_recv,
    ssq_sem,
):
    row, z, c = lax.axis_index("row"), lax.axis_index("col"), lax.axis_index("depth")
    rows, width = halves.shape[1], halves.shape[2]
    tiles = width // LANES
    cols = out.shape[2]
    kblocks = cols // LANES
    half = rows // 2
    other = 1 - c
    first, last = row == 0, row == nrow - 1
    edge = jnp.logical_or(first, last)

    def copy_out(src, dst, send, recv, where):
        return pltpu.make_async_remote_copy(
            src_ref=src, dst_ref=dst, send_sem=send, recv_sem=recv, device_id=where, device_id_type=MESH
        )

    own = pl.ds(pl.multiple_of(c * width, width), width)
    sources = [
        (spectrum.at[:, 0], tab.at[c, z, 0]),
        (spectrum.at[:, 1], tab.at[c, z, 1]),
        (wanted.at[c], want.at[z]),
        (fraction.at[c], frac.at[z]),
        (halves.at[0, pl.ds(rows - 8, 8)], edges.at[0]),
        (halves.at[1, pl.ds(0, 8)], edges.at[1]),
    ]
    local = [pltpu.make_async_copy(src, dst, local_sem.at[k]) for k, (src, dst) in enumerate(sources)]
    for d in local:
        d.start()
    a_local = pltpu.make_async_copy(halves, afull.at[:, :, own], a_sem.at[0])
    a_local.start()

    barrier = pltpu.get_barrier_semaphore()

    def greet(where):
        pl.semaphore_signal(barrier, inc=1, device_id=where, device_id_type=MESH)

    order = sorted(range(1, n), key=lambda o: -min(o, n - o))
    for o in order:
        zz = lax.rem(z + o, n)
        greet((row, zz, c))
    greet((row, z, other))

    @pl.when(edge)
    def _():
        def one(i, carry):
            rr = lax.rem(row + i, nrow)
            greet((rr, z, c))
            greet((rr, z, other))
            return carry

        lax.fori_loop(1, nrow, one, 0)

    @pl.when(jnp.logical_not(edge))
    def _():
        for rr in (0, nrow - 1):
            greet((rr, z, c))
            greet((rr, z, other))

    for d in local:
        d.wait()

    def spread(rows_of, target, a, dp):
        turned = rows_of.T
        for s in range(tiles):
            at = pl.multiple_of(dp * width + s * LANES, LANES)
            target[a, pl.ds(at, LANES), :] = jnp.broadcast_to(turned[:, s : s + 1], (LANES, LANES))

    for a in range(2):
        line = edges[a].astype(jnp.float32)
        line = line[7:8] if a == 0 else line[0:1]
        for s in range(tiles):
            edge_row[a, s : s + 1, :] = line[:, s * LANES : (s + 1) * LANES]
    for a in range(2):
        spread(tab[c, z, a], specb, a, c)

    pl.semaphore_wait(barrier, n + jnp.where(edge, 2 * (nrow - 1), 4))

    for o in order:
        where = (row, lax.rem(z + o, n), c)
        for ref, sem in ((tab.at[c, z], tab_sem), (want.at[z], want_sem), (frac.at[z], frac_sem)):
            copy_out(ref, ref, sem.at[0], sem.at[1], where).start()

    def seam_copy(a, i, where_c):
        return copy_out(
            edge_row.at[a],
            seam.at[c, a],
            seam_send,
            seam_recv,
            (lax.rem(row + i, nrow), z, where_c),
        )

    for flag, a in ((last, 0), (first, 1)):

        @pl.when(flag)
        def _(a=a):
            def one(i, carry):
                seam_copy(a, i, 0).start()
                seam_copy(a, i, 1).start()
                return carry

            pltpu.make_async_copy(edge_row.at[a], seam.at[c, a], seam_recv).start()
            seam_copy(a, 0, other).start()
            lax.fori_loop(1, nrow, one, 0)

    near_copy = copy_out(tab.at[c, z], near, tab_sem.at[4], tab_sem.at[5], (row, z, other))
    near_copy.start()

    a_swap = [
        copy_out(halves.at[a], afull.at[a, :, own], a_sem.at[1 + a], a_sem.at[3 + a], (row, z, other))
        for a in range(2)
    ]
    for d in a_swap:
        d.start()

    def arrived(ref, sem):
        pltpu.make_async_copy(ref, ref, sem).wait()

    near_copy.wait_recv()

    def onward(o):
        return copy_out(near, tab.at[0, z], tab_sem.at[6], tab_sem.at[2], (row, lax.rem(z + o, n), c))

    @pl.when(c == 1)
    def _():
        for o in order:
            onward(o).start()

    for a in range(2):
        spread(near[a], specb, a, other)

    others = pl.ds(0, n - 1)
    arrived(tab.at[c, others], tab_sem.at[1])
    tab_swap = copy_out(tab.at[1], tab.at[1], tab_sem.at[3], tab_sem.at[2], (row, z, 0))

    @pl.when(c == 1)
    def _():
        tab_swap.start()
        tab[0, z] = near[...]

    pairs = [(dp, a) for dp in range(2) for a in range(2)]
    arrived(seam, seam_recv)
    for dp in range(2):
        spread(seam[dp, 0], seamb, 0, dp)
    arrived(want.at[others], want_sem.at[1])
    arrived(frac.at[others], frac_sem.at[1])

    @pl.when(c == 0)
    def _():
        arrived(tab.at[1], tab_sem.at[2])

    @pl.when(c == 1)
    def _():
        arrived(tab.at[0, others], tab_sem.at[2])


    table = (tab[...].reshape(4 * n * tiles, LANES) * 0.25).T
    hi = table.astype(jnp.bfloat16)
    rest = table - hi.astype(jnp.float32)
    mid = rest.astype(jnp.bfloat16)
    low = (rest - mid.astype(jnp.float32)).astype(jnp.bfloat16)
    tcat[0:LANES] = hi
    tcat[LANES : 2 * LANES] = mid
    tcat[2 * LANES : 3 * LANES] = low

    def pick(position):
        h = lax.shift_right_logical(position, 1)
        a = position & 1
        g = lax.shift_right_logical(h, log2(width))
        s = lax.shift_right_logical(h, log2(LANES)) & (tiles - 1)
        entry = (((g & 1) * n + lax.shift_right_logical(g, 1)) * 2 + a) * tiles + s
        lane = h & (LANES - 1)
        hit = lax.broadcasted_iota(jnp.int32, (tcat.shape[1], cols), 0) == entry
        onehot = jnp.where(hit, 1.0, 0.0).astype(jnp.bfloat16)
        found = jnp.dot(tcat[...], onehot, preferred_element_type=jnp.float32)
        value = (found[0:LANES] + found[LANES : 2 * LANES]) + found[2 * LANES : 3 * LANES]
        here = lax.broadcasted_iota(jnp.int32, (LANES, cols), 0) == lane
        return jnp.sum(jnp.where(here, value, 0.0), axis=0, keepdims=True) * 4.0

    def roots(d):
        def line(ref):
            block = ref[d]
            return jnp.concatenate([block[b : b + 1] for b in range(kblocks)], axis=1)

        position = line(want)
        lower = pick(position)
        upper = pick(position + 1)
        return lower, line(frac) * (upper - lower)

    def at_offset(off):
        return lax.rem(z + off + n, n)

    def ssq_copy(off):
        return copy_out(
            ssq_s.at[lax.rem(off + n, n)], ssq_r.at[z], ssq_sem.at[0], ssq_sem.at[1], (row, at_offset(off), c)
        )

    step_rows = 64

    def cauchy(a, lower, scaled, carry):
        def one(t, carry):
            at = pl.ds(t * step_rows, step_rows)
            value = specb[a, at, :]
            weight = seamb[a, at, :]
            sums = []
            for b in range(kblocks):
                lanes = slice(b * LANES, (b + 1) * LANES)
                term = weight / ((value - lower[:, lanes]) - scaled[:, lanes])
                ct[at, lanes] = term.astype(jnp.bfloat16)
                squares = (term * term).reshape(step_rows // 8, 8, LANES)
                sums.append(carry[b] + jnp.sum(squares, axis=0))
            return tuple(sums)

        for t in range(2 * width // step_rows):
            carry = one(t, carry)
        return carry

    def product(slot, a):
        part[slot, a] = jnp.dot(afull[a], ct[...], preferred_element_type=jnp.float32)

    steps = n - 1
    m = n // 2

    def ring_copy(j, way, a):
        step = 1 if way == 0 else n - 1
        return copy_out(
            sbuf.at[j, way, a],
            rbuf.at[j, way, a],
            ring_send,
            ring_recv.at[j, way],
            (row, lax.rem(z + step, n), c),
        )

    def mine(j, way, a):
        off = m - lax.div(j + 1, 2)
        slot = off if way == 0 else lax.rem(n - off, n)
        start = pl.multiple_of(lax.rem(j + way, 2) * half, half)
        return part[slot, a, pl.ds(start, half), :]

    def launch(j, way, a):
        sbuf[j, way, a] = mine(j, way, a).astype(jnp.bfloat16)
        ring_copy(j, way, a).start()

    def relay(j, way, a):
        total = mine(j, way, a) + rbuf[j - 2, way, a].astype(jnp.float32)
        sbuf[j, way, a] = total.astype(jnp.bfloat16)
        ring_copy(j, way, a).start()

    def unit(u, carry):
        ends = jnp.logical_or(u < 2, u >= 2 * n - 2)
        pair = jnp.where(ends, jnp.where(u < 2, 0, m), lax.div(u + 2, 4))
        turn = jnp.where(ends, 0, lax.rem(u, 2))
        a = jnp.where(ends, lax.rem(u, 2), lax.div(lax.rem(u + 2, 4), 2))
        off = jnp.where(turn == 0, m - pair, pair - m)
        slot = lax.rem(off + n, n)

        @pl.when(a == 0)
        def _():
            lower, scaled = roots(at_offset(off))
            root[turn, 0] = lower
            root[turn, 1] = scaled
            ssq[turn] = jnp.zeros(ssq.shape[1:], jnp.float32)

        sums = cauchy(a, root[turn, 0], root[turn, 1], tuple(ssq[turn, b] for b in range(kblocks)))
        product(slot, a)
        for b in range(kblocks):
            ssq[turn, b] = sums[b]

        @pl.when(jnp.logical_and(c == 0, u == 2))
        def _():
            def both(k, carry):
                for way in range(2):
                    launch(0, way, k)
                return carry

            lax.fori_loop(0, 2, both, 0)

        for way in range(2):
            first = jnp.logical_or(
                jnp.logical_and(u < 2, c == 1), jnp.logical_and(pair == 1, turn == way)
            )

            @pl.when(first)
            def _(way=way):
                launch(jnp.minimum(pair, 1), way, a)

        @pl.when(u == 0)
        def _():
            for dp in range(2):
                spread(seam[dp, 1], seamb, 1, dp)

        @pl.when(a == 1)
        def _():
            for b in range(kblocks):
                ssq_s[slot, b : b + 1, :] = jnp.sum(ssq[turn, b], axis=0, keepdims=True)

            @pl.when(u < 2 * n - 1)
            def _():
                ssq_copy(off).start()

        @pl.when(jnp.logical_and(lax.rem(u, 4) == 1, jnp.logical_and(u >= 5, u < 2 * n - 2)))
        def _():
            relays(lax.div(u + 3, 4))

        return carry

    def relays(j):
        for way in range(2):
            arrived(rbuf.at[j - 2, way], ring_recv.at[j - 2, way])

            def each(a, carry, way=way):
                relay(j, way, a)
                return carry

            lax.fori_loop(0, 2, each, 0)

    a_local.wait()
    for d in a_swap:
        d.wait_recv()
    lax.fori_loop(0, 2 * n, unit, 0)

    def rest(j, carry):
        relays(j)
        return carry

    lax.fori_loop(m + 1, steps, rest, 0)

    for ref, sem in ((tab.at[c, others], tab_sem), (want.at[others], want_sem), (frac.at[others], frac_sem)):
        arrived(ref, sem.at[0])
    arrived(ssq_s.at[others], ssq_sem.at[0])

    @pl.when(c == 1)
    def _():
        tab_swap.wait_send()
        arrived(tab.at[0, others], tab_sem.at[6])

    for d in a_swap:
        d.wait_send()
    near_copy.wait_send()
    for flag in (last, first):

        @pl.when(flag)
        def _():
            arrived(specb.at[0, pl.ds(0, (2 * nrow - 1) * tiles), :], seam_send)

    arrived(ssq_r.at[others], ssq_sem.at[1])
    total = ssq_s[0]
    for o in range(1, n):
        total = total + ssq_r[lax.rem(z + o, n)]
    norm = jnp.sqrt(total)
    norm = jnp.concatenate([norm[b : b + 1] for b in range(kblocks)], axis=1)
    inverse = 1.0 / norm

    def landed(j, way):
        arrived(rbuf.at[j, way], ring_recv.at[j, way])
        hh = (j + way) % 2
        return slice(hh * half, (hh + 1) * half), rbuf[j, way].astype(jnp.float32)

    for way in range(2):
        at, value = landed(steps - 2, way)
        part[0, :, at, :] += value
    for way in range(2):
        at, value = landed(steps - 1, way)
        out[:, at, :] = (part[0, :, at, :] + value) * inverse

    arrived(sbuf, ring_send)


def merge(nrow, n, halves, spectrum, wanted, fraction):
    rows, width = halves.shape[1:]
    tiles = width // LANES
    cols = wanted.shape[0] // 2
    kblocks = cols // LANES
    spectrum = spectrum.reshape(2, tiles, LANES).transpose(1, 0, 2)
    operands = (halves, spectrum, wanted.reshape(2, kblocks, LANES), fraction.reshape(2, kblocks, LANES))
    half = rows // 2
    steps = n - 1
    bf16, f32 = jnp.bfloat16, jnp.float32
    return pl.pallas_call(
        functools.partial(kernel, nrow, n),
        out_shape=jax.ShapeDtypeStruct((2, rows, cols), f32),
        in_specs=[pl.BlockSpec(memory_space=pltpu.HBM)] * 4,
        out_specs=pl.BlockSpec(memory_space=pltpu.VMEM),
        scratch_shapes=[
            pltpu.VMEM((2, rows, 2 * width), bf16),
            pltpu.VMEM((2, 8, width), bf16),
            pltpu.VMEM((2, tiles, LANES), f32),
            pltpu.VMEM((2, n, 2, tiles, LANES), f32),
            pltpu.VMEM((2, tiles, LANES), f32),
            pltpu.VMEM((n, kblocks, LANES), jnp.int32),
            pltpu.VMEM((n, kblocks, LANES), f32),
            pltpu.VMEM((2, 2, tiles, LANES), f32),
            pltpu.VMEM((2, 2 * width, LANES), f32),
            pltpu.VMEM((2, 2 * width, LANES), f32),
            pltpu.VMEM((3 * LANES, 4 * n * tiles), bf16),
            pltpu.VMEM((2 * width, cols), bf16),
            pltpu.VMEM((2, 2, 1, cols), f32),
            pltpu.VMEM((2, kblocks, 8, LANES), f32),
            pltpu.VMEM((n, 2, rows, cols), f32),
            pltpu.VMEM((steps, 2, 2, half, cols), bf16),
            pltpu.VMEM((steps, 2, 2, half, cols), bf16),
            pltpu.VMEM((n, kblocks, LANES), f32),
            pltpu.VMEM((n, kblocks, LANES), f32),
            pltpu.SemaphoreType.DMA((5,)),
            pltpu.SemaphoreType.DMA((6,)),
            pltpu.SemaphoreType.DMA((7,)),
            pltpu.SemaphoreType.DMA((2,)),
            pltpu.SemaphoreType.DMA((2,)),
            pltpu.SemaphoreType.DMA,
            pltpu.SemaphoreType.DMA,
            pltpu.SemaphoreType.DMA,
            pltpu.SemaphoreType.DMA((steps, 2)),
            pltpu.SemaphoreType.DMA((2,)),
        ],
        compiler_params=pltpu.CompilerParams(
            collective_id=0, has_side_effects=True, vmem_limit_bytes=48 * 1024 * 1024
        ),
        name="merge",
    )(*[pltpu.with_memory_space_constraint(x, pltpu.HBM) for x in operands])


def solution(mesh):
    body = functools.partial(merge, mesh.shape["row"], mesh.shape["col"])
    in_specs = (P(None, "row", ("col", "depth")), P(None, ("col", "depth")), P("col"), P("col"))
    out_specs = P(None, "row", ("col", "depth"))
    return jax.shard_map(body, mesh=mesh, in_specs=in_specs, out_specs=out_specs, check_vma=False)
```

```python
import functools

import jax
import jax.numpy as jnp
from jax import lax
from jax.experimental import pallas as pl
from jax.experimental.pallas import tpu as pltpu
from jax.sharding import PartitionSpec as P

MESH = pl.DeviceIdType.MESH
LANES = 128


def log2(x):
    return x.bit_length() - 1


def kernel(
    nrow,
    n,
    halves,
    spectrum,
    wanted,
    fraction,
    out,
    afull,
    edges,
    edge_row,
    tab,
    near,
    want,
    frac,
    seam,
    specb,
    seamb,
    tcat,
    ct,
    root,
    ssq,
    part,
    sbuf,
    rbuf,
    ssq_s,
    ssq_r,
    a_sem,
    local_sem,
    tab_sem,
    want_sem,
    frac_sem,
    seam_send,
    seam_recv,
    ring_send,
    ring_recv,
    ssq_sem,
):
    row, z, c = lax.axis_index("row"), lax.axis_index("col"), lax.axis_index("depth")
    rows, width = halves.shape[1], halves.shape[2]
    tiles = width // LANES
    cols = out.shape[2]
    kblocks = cols // LANES
    half = rows // 2
    other = 1 - c
    first, last = row == 0, row == nrow - 1
    edge = jnp.logical_or(first, last)

    def copy_out(src, dst, send, recv, where):
        return pltpu.make_async_remote_copy(
            src_ref=src, dst_ref=dst, send_sem=send, recv_sem=recv, device_id=where, device_id_type=MESH
        )

    own = pl.ds(pl.multiple_of(c * width, width), width)
    sources = [
        (spectrum.at[:, 0], tab.at[c, z, 0]),
        (spectrum.at[:, 1], tab.at[c, z, 1]),
        (wanted.at[c], want.at[z]),
        (fraction.at[c], frac.at[z]),
        (halves.at[0, pl.ds(rows - 8, 8)], edges.at[0]),
        (halves.at[1, pl.ds(0, 8)], edges.at[1]),
    ]
    local = [pltpu.make_async_copy(src, dst, local_sem.at[k]) for k, (src, dst) in enumerate(sources)]
    for d in local:
        d.start()
    a_local = pltpu.make_async_copy(halves, afull.at[:, :, own], a_sem.at[0])
    a_local.start()

    barrier = pltpu.get_barrier_semaphore()

    def greet(where):
        pl.semaphore_signal(barrier, inc=1, device_id=where, device_id_type=MESH)

    order = sorted(range(1, n), key=lambda o: -min(o, n - o))
    for o in order:
        zz = lax.rem(z + o, n)
        greet((row, zz, c))
    greet((row, z, other))

    @pl.when(edge)
    def _():
        def one(i, carry):
            rr = lax.rem(row + i, nrow)
            greet((rr, z, c))
            greet((rr, z, other))
            return carry

        lax.fori_loop(1, nrow, one, 0)

    @pl.when(jnp.logical_not(edge))
    def _():
        for rr in (0, nrow - 1):
            greet((rr, z, c))
            greet((rr, z, other))

    for d in local:
        d.wait()

    def spread(rows_of, target, a, dp):
        turned = rows_of.T
        for s in range(tiles):
            at = pl.multiple_of(dp * width + s * LANES, LANES)
            target[a, pl.ds(at, LANES), :] = jnp.broadcast_to(turned[:, s : s + 1], (LANES, LANES))

    for a in range(2):
        line = edges[a].astype(jnp.float32)
        line = line[7:8] if a == 0 else line[0:1]
        for s in range(tiles):
            edge_row[a, s : s + 1, :] = line[:, s * LANES : (s + 1) * LANES]
    for a in range(2):
        spread(tab[c, z, a], specb, a, c)

    pl.semaphore_wait(barrier, n + jnp.where(edge, 2 * (nrow - 1), 4))

    for o in order:
        where = (row, lax.rem(z + o, n), c)
        for ref, sem in ((tab.at[c, z], tab_sem), (want.at[z], want_sem), (frac.at[z], frac_sem)):
            copy_out(ref, ref, sem.at[0], sem.at[1], where).start()

    def seam_copy(a, i, where_c):
        return copy_out(
            edge_row.at[a],
            seam.at[c, a],
            seam_send,
            seam_recv,
            (lax.rem(row + i, nrow), z, where_c),
        )

    for flag, a in ((last, 0), (first, 1)):

        @pl.when(flag)
        def _(a=a):
            def one(i, carry):
                seam_copy(a, i, 0).start()
                seam_copy(a, i, 1).start()
                return carry

            pltpu.make_async_copy(edge_row.at[a], seam.at[c, a], seam_recv).start()
            seam_copy(a, 0, other).start()
            lax.fori_loop(1, nrow, one, 0)

    near_copy = copy_out(tab.at[c, z], near, tab_sem.at[4], tab_sem.at[5], (row, z, other))
    near_copy.start()

    a_swap = [
        copy_out(halves.at[a], afull.at[a, :, own], a_sem.at[1 + a], a_sem.at[3 + a], (row, z, other))
        for a in range(2)
    ]
    for d in a_swap:
        d.start()

    def arrived(ref, sem):
        pltpu.make_async_copy(ref, ref, sem).wait()

    near_copy.wait_recv()

    def onward(o):
        return copy_out(near, tab.at[0, z], tab_sem.at[6], tab_sem.at[2], (row, lax.rem(z + o, n), c))

    @pl.when(c == 1)
    def _():
        for o in order:
            onward(o).start()

    for a in range(2):
        spread(near[a], specb, a, other)

    others = pl.ds(0, n - 1)
    arrived(tab.at[c, others], tab_sem.at[1])
    tab_swap = copy_out(tab.at[1], tab.at[1], tab_sem.at[3], tab_sem.at[2], (row, z, 0))

    @pl.when(c == 1)
    def _():
        tab_swap.start()
        tab[0, z] = near[...]

    pairs = [(dp, a) for dp in range(2) for a in range(2)]
    arrived(seam, seam_recv)
    for dp in range(2):
        spread(seam[dp, 0], seamb, 0, dp)
    arrived(want.at[others], want_sem.at[1])
    arrived(frac.at[others], frac_sem.at[1])

    @pl.when(c == 0)
    def _():
        arrived(tab.at[1], tab_sem.at[2])

    @pl.when(c == 1)
    def _():
        arrived(tab.at[0, others], tab_sem.at[2])


    table = (tab[...].reshape(4 * n * tiles, LANES) * 0.25).T
    hi = table.astype(jnp.bfloat16)
    rest = table - hi.astype(jnp.float32)
    mid = rest.astype(jnp.bfloat16)
    low = (rest - mid.astype(jnp.float32)).astype(jnp.bfloat16)
    tcat[0:LANES] = hi
    tcat[LANES : 2 * LANES] = mid
    tcat[2 * LANES : 3 * LANES] = low

    def pick(position):
        h = lax.shift_right_logical(position, 1)
        a = position & 1
        g = lax.shift_right_logical(h, log2(width))
        s = lax.shift_right_logical(h, log2(LANES)) & (tiles - 1)
        entry = (((g & 1) * n + lax.shift_right_logical(g, 1)) * 2 + a) * tiles + s
        lane = h & (LANES - 1)
        hit = lax.broadcasted_iota(jnp.int32, (tcat.shape[1], cols), 0) == entry
        onehot = jnp.where(hit, 1.0, 0.0).astype(jnp.bfloat16)
        found = jnp.dot(tcat[...], onehot, preferred_element_type=jnp.float32)
        value = (found[0:LANES] + found[LANES : 2 * LANES]) + found[2 * LANES : 3 * LANES]
        here = lax.broadcasted_iota(jnp.int32, (LANES, cols), 0) == lane
        return jnp.sum(jnp.where(here, value, 0.0), axis=0, keepdims=True) * 4.0

    def roots(d):
        def line(ref):
            block = ref[d]
            return jnp.concatenate([block[b : b + 1] for b in range(kblocks)], axis=1)

        position = line(want)
        lower = pick(position)
        upper = pick(position + 1)
        return lower, line(frac) * (upper - lower)

    def at_offset(off):
        return lax.rem(z + off + n, n)

    def ssq_copy(off):
        return copy_out(
            ssq_s.at[lax.rem(off + n, n)], ssq_r.at[z], ssq_sem.at[0], ssq_sem.at[1], (row, at_offset(off), c)
        )

    step_rows = 64

    def cauchy(a, lower, scaled, carry):
        def one(t, carry):
            at = pl.ds(t * step_rows, step_rows)
            value = specb[a, at, :]
            weight = seamb[a, at, :]
            sums = []
            for b in range(kblocks):
                lanes = slice(b * LANES, (b + 1) * LANES)
                term = weight / ((value - lower[:, lanes]) - scaled[:, lanes])
                ct[at, lanes] = term.astype(jnp.bfloat16)
                squares = (term * term).reshape(step_rows // 8, 8, LANES)
                sums.append(carry[b] + jnp.sum(squares, axis=0))
            return tuple(sums)

        for t in range(2 * width // step_rows):
            carry = one(t, carry)
        return carry

    def product(slot, a):
        part[slot, a] = jnp.dot(afull[a], ct[...], preferred_element_type=jnp.float32)

    steps = n - 1
    m = n // 2

    def ring_copy(j, way, a):
        step = 1 if way == 0 else n - 1
        return copy_out(
            sbuf.at[j, way, a],
            rbuf.at[j, way, a],
            ring_send,
            ring_recv.at[j, way],
            (row, lax.rem(z + step, n), c),
        )

    def mine(j, way, a):
        off = m - lax.div(j + 1, 2)
        slot = off if way == 0 else lax.rem(n - off, n)
        start = pl.multiple_of(lax.rem(j + way, 2) * half, half)
        return part[slot, a, pl.ds(start, half), :]

    def launch(j, way, a):
        sbuf[j, way, a] = mine(j, way, a).astype(jnp.bfloat16)
        ring_copy(j, way, a).start()

    def relay(j, way, a):
        total = mine(j, way, a) + rbuf[j - 2, way, a].astype(jnp.float32)
        sbuf[j, way, a] = total.astype(jnp.bfloat16)
        ring_copy(j, way, a).start()

    def unit(u, carry):
        ends = jnp.logical_or(u < 2, u >= 2 * n - 2)
        pair = jnp.where(ends, jnp.where(u < 2, 0, m), lax.div(u + 2, 4))
        turn = jnp.where(ends, 0, lax.rem(u, 2))
        a = jnp.where(ends, lax.rem(u, 2), lax.div(lax.rem(u + 2, 4), 2))
        off = jnp.where(turn == 0, m - pair, pair - m)
        slot = lax.rem(off + n, n)

        @pl.when(a == 0)
        def _():
            lower, scaled = roots(at_offset(off))
            root[turn, 0] = lower
            root[turn, 1] = scaled
            ssq[turn] = jnp.zeros(ssq.shape[1:], jnp.float32)

        sums = cauchy(a, root[turn, 0], root[turn, 1], tuple(ssq[turn, b] for b in range(kblocks)))
        product(slot, a)
        for b in range(kblocks):
            ssq[turn, b] = sums[b]

        @pl.when(jnp.logical_and(c == 0, jnp.logical_or(u == 2, u == 3)))
        def _():
            for way in range(2):
                launch(0, way, u - 2)

        for way in range(2):
            first = jnp.logical_or(
                jnp.logical_and(u < 2, c == 1), jnp.logical_and(pair == 1, turn == way)
            )

            @pl.when(first)
            def _(way=way):
                launch(jnp.minimum(pair, 1), way, a)

        @pl.when(u == 0)
        def _():
            for dp in range(2):
                spread(seam[dp, 1], seamb, 1, dp)

        @pl.when(a == 1)
        def _():
            for b in range(kblocks):
                ssq_s[slot, b : b + 1, :] = jnp.sum(ssq[turn, b], axis=0, keepdims=True)

            @pl.when(u < 2 * n - 1)
            def _():
                ssq_copy(off).start()

        @pl.when(jnp.logical_and(lax.rem(u, 4) == 1, jnp.logical_and(u >= 5, u < 2 * n - 2)))
        def _():
            relays(lax.div(u + 3, 4))

        return carry

    def relays(j):
        for way in range(2):
            arrived(rbuf.at[j - 2, way], ring_recv.at[j - 2, way])

            def each(a, carry, way=way):
                relay(j, way, a)
                return carry

            lax.fori_loop(0, 2, each, 0)

    a_local.wait()
    for d in a_swap:
        d.wait_recv()
    lax.fori_loop(0, 2 * n, unit, 0)

    def rest(j, carry):
        relays(j)
        return carry

    lax.fori_loop(m + 1, steps, rest, 0)

    for ref, sem in ((tab.at[c, others], tab_sem), (want.at[others], want_sem), (frac.at[others], frac_sem)):
        arrived(ref, sem.at[0])
    arrived(ssq_s.at[others], ssq_sem.at[0])

    @pl.when(c == 1)
    def _():
        tab_swap.wait_send()
        arrived(tab.at[0, others], tab_sem.at[6])

    for d in a_swap:
        d.wait_send()
    near_copy.wait_send()
    for flag in (last, first):

        @pl.when(flag)
        def _():
            arrived(specb.at[0, pl.ds(0, (2 * nrow - 1) * tiles), :], seam_send)

    arrived(ssq_r.at[others], ssq_sem.at[1])
    total = ssq_s[0]
    for o in range(1, n):
        total = total + ssq_r[lax.rem(z + o, n)]
    norm = jnp.sqrt(total)
    norm = jnp.concatenate([norm[b : b + 1] for b in range(kblocks)], axis=1)
    inverse = 1.0 / norm

    def landed(j, way):
        arrived(rbuf.at[j, way], ring_recv.at[j, way])
        hh = (j + way) % 2
        return slice(hh * half, (hh + 1) * half), rbuf[j, way].astype(jnp.float32)

    for way in range(2):
        at, value = landed(steps - 2, way)
        part[0, :, at, :] += value
    for way in range(2):
        at, value = landed(steps - 1, way)
        out[:, at, :] = (part[0, :, at, :] + value) * inverse

    arrived(sbuf, ring_send)


def merge(nrow, n, halves, spectrum, wanted, fraction):
    rows, width = halves.shape[1:]
    tiles = width // LANES
    cols = wanted.shape[0] // 2
    kblocks = cols // LANES
    spectrum = spectrum.reshape(2, tiles, LANES).transpose(1, 0, 2)
    operands = (halves, spectrum, wanted.reshape(2, kblocks, LANES), fraction.reshape(2, kblocks, LANES))
    half = rows // 2
    steps = n - 1
    bf16, f32 = jnp.bfloat16, jnp.float32
    return pl.pallas_call(
        functools.partial(kernel, nrow, n),
        out_shape=jax.ShapeDtypeStruct((2, rows, cols), f32),
        in_specs=[pl.BlockSpec(memory_space=pltpu.HBM)] * 4,
        out_specs=pl.BlockSpec(memory_space=pltpu.VMEM),
        scratch_shapes=[
            pltpu.VMEM((2, rows, 2 * width), bf16),
            pltpu.VMEM((2, 8, width), bf16),
            pltpu.VMEM((2, tiles, LANES), f32),
            pltpu.VMEM((2, n, 2, tiles, LANES), f32),
            pltpu.VMEM((2, tiles, LANES), f32),
            pltpu.VMEM((n, kblocks, LANES), jnp.int32),
            pltpu.VMEM((n, kblocks, LANES), f32),
            pltpu.VMEM((2, 2, tiles, LANES), f32),
            pltpu.VMEM((2, 2 * width, LANES), f32),
            pltpu.VMEM((2, 2 * width, LANES), f32),
            pltpu.VMEM((3 * LANES, 4 * n * tiles), bf16),
            pltpu.VMEM((2 * width, cols), bf16),
            pltpu.VMEM((2, 2, 1, cols), f32),
            pltpu.VMEM((2, kblocks, 8, LANES), f32),
            pltpu.VMEM((n, 2, rows, cols), f32),
            pltpu.VMEM((steps, 2, 2, half, cols), bf16),
            pltpu.VMEM((steps, 2, 2, half, cols), bf16),
            pltpu.VMEM((n, kblocks, LANES), f32),
            pltpu.VMEM((n, kblocks, LANES), f32),
            pltpu.SemaphoreType.DMA((5,)),
            pltpu.SemaphoreType.DMA((6,)),
            pltpu.SemaphoreType.DMA((7,)),
            pltpu.SemaphoreType.DMA((2,)),
            pltpu.SemaphoreType.DMA((2,)),
            pltpu.SemaphoreType.DMA,
            pltpu.SemaphoreType.DMA,
            pltpu.SemaphoreType.DMA,
            pltpu.SemaphoreType.DMA((steps, 2)),
            pltpu.SemaphoreType.DMA((2,)),
        ],
        compiler_params=pltpu.CompilerParams(
            collective_id=0, has_side_effects=True, vmem_limit_bytes=48 * 1024 * 1024
        ),
        name="merge",
    )(*[pltpu.with_memory_space_constraint(x, pltpu.HBM) for x in operands])


def solution(mesh):
    body = functools.partial(merge, mesh.shape["row"], mesh.shape["col"])
    in_specs = (P(None, "row", ("col", "depth")), P(None, ("col", "depth")), P("col"), P("col"))
    out_specs = P(None, "row", ("col", "depth"))
    return jax.shard_map(body, mesh=mesh, in_specs=in_specs, out_specs=out_specs, check_vma=False)
```
